128 devices in a mesh: branch: 4 (over z_lo, core), query: 32 (over z_hi, x, y).
Axes of the slice: x: 4, y: 4, z: 4 (z_hi: 2, z_lo: 2; z = z_hi * 2 + z_lo), core: 2. Of those that a mesh axis runs over, the one named last changes fastest.
Arguments:
- sensors: bfloat16 [3, 128, 2048], P(None, ('branch', 'query')), may hold values from -24 to 24
- branch_w: bfloat16 [3, 2048, 1024], replicated, may hold values from -0.125 to 0.125
- branch_b: float32 [3, 1024], replicated, may hold values from -3 to 3
- coords: bfloat16 [3, 65536], P(None, ('branch', 'query')), may hold values from -1 to 1
- func_index: int32 [65536], P(('branch', 'query')), may hold values from 0 to 31
- targets: float32 [65536], P(('branch', 'query')), may hold values from -6 to 6
- trunk_w1: bfloat16 [3, 1024], replicated, may hold values from -3.5 to 3.5
- trunk_b1: float32 [1024], replicated, may hold values from -3 to 3
- trunk_w2: bfloat16 [1024, 1024], replicated, may hold values from -0.1875 to 0.1875
- trunk_b2: float32 [1024], replicated, may hold values from -3 to 3
Outputs:
- grad_branch_w: float32 [3, 2048, 1024], P(None, 'query')
- grad_branch_b: float32 [3, 1024], replicated
- grad_trunk_w1: float32 [3, 1024], replicated
- grad_trunk_b1: float32 [1024], replicated
- grad_trunk_w2: float32 [1024, 1024], replicated
- grad_trunk_b2: float32 [1024], replicated
The draws below stay inside these ranges and needn't reach their ends.
Inputs may be any that keep to these rules, and one draw needn't show every extreme that they name: func_index[i] names one of the 32 function samples whose rows of sensors stand in the same owner group (index of the mesh axis branch) as query point i.
All inputs are finite; a program needn't handle non-finite values.
Results may differ from the reference program's by a relative error of at most 0.018.
Values may be sent and summed in bfloat16 or wider, within the bound.
A program may use at most 128 MiB of HBM per device.

```python
import jax
import jax.numpy as jnp
from jax import lax

BRANCHES = 3
DIMS = 3
SENSORS = 2048
LATENT = 1024
HIDDEN_SIZE = 1024
QRY_DEV = 512
GROUP_FUNCS = 32
FUNCS = 128
QUERIES = 65536
N_QUERY = 32


def with_ends(result, key, least, largest):
    extent = result.shape
    index_at = [jax.random.randint(jax.random.fold_in(key, axis), (), 0, extent[axis]) for axis in range(len(extent))]
    result = result.at[tuple(index_at)].set(least)
    longest = extent.index(max(extent))
    index_at[longest] = (index_at[longest] + 1) % extent[longest]
    return result.at[tuple(index_at)].set(largest)


def spiked(entries, rng, source, target, shards_of, factor):
    def block_of(axis_at):
        return (jnp.arange(entries.shape[axis_at]) // (entries.shape[axis_at] // shards_of)).reshape((-1,) + (1,) * (entries.ndim - 1 - axis_at))

    one_side = jax.random.permutation(rng, shards_of)[block_of(target)]
    second = (block_of(target) + shards_of // 2) % shards_of
    return jnp.where((block_of(source) == one_side) | (block_of(source) == second), factor * entries, entries)


def steps_of(key, shape, shards, low, high):
    level = 1.0
    for axis_at, parts in shards:
        draws = jax.random.uniform(jax.random.fold_in(jax.random.fold_in(key, 6), axis_at), (parts,), jnp.float32, low / len(shards), high / len(shards))
        level = level * jnp.repeat(jnp.exp(draws), shape[axis_at] // parts).reshape((-1,) + (1,) * (len(shape) - 1 - axis_at))
    return level


def bell_draw(key, shape, width, most, pieces=(), held_as=jnp.bfloat16):
    gain = steps_of(key, shape, pieces, -0.22, 0.18) if pieces else 1.0
    array = jax.random.normal(key, shape, jnp.float32) * width * gain
    return jnp.minimum(jnp.maximum(array, -most), most).astype(held_as)


def gaussian_with(key, extent, spread, most, split, heavy, kind=jnp.bfloat16):
    entries = spread * jax.random.normal(key, extent, jnp.float32)
    if split:
        entries = entries * steps_of(key, extent, split, -0.22, 0.18)
    return jnp.clip(spiked(entries, jax.random.fold_in(key, 3), *heavy), -most, most).astype(kind)


def setup_inputs(seed: int = 0) -> dict:
    splits = jax.random.split(jax.random.key(seed), 11)
    return {
        "sensors": gaussian_with(splits[0], (BRANCHES, FUNCS, SENSORS), 1.0, 24.0, ((1, 128),), (1, 2, 128, 5.5)),
        "branch_w": bell_draw(splits[1], (BRANCHES, SENSORS, LATENT), SENSORS ** -0.5, 0.125),
        "branch_b": bell_draw(splits[2], (BRANCHES, LATENT), 0.5, 3.0, (), jnp.float32),
        "coords": jnp.clip(jax.random.uniform(splits[3], (DIMS, QUERIES), jnp.float32, -1.0, 1.0) * steps_of(splits[3], (DIMS, QUERIES), ((1, 128),), -0.4, 0.0), -1.0, 1.0).astype(jnp.bfloat16),
        "func_index": with_ends(jax.random.randint(splits[4], (QUERIES,), 0, GROUP_FUNCS), jax.random.fold_in(splits[4], 1), 0, GROUP_FUNCS - 1).astype(jnp.int32),
        "targets": bell_draw(splits[5], (QUERIES,), 1.0, 6.0, ((0, 128),), jnp.float32),
        "trunk_w1": bell_draw(splits[6], (DIMS, HIDDEN_SIZE), DIMS ** -0.5, 3.5),
        "trunk_b1": bell_draw(splits[7], (HIDDEN_SIZE,), 0.5, 3.0, (), jnp.float32),
        "trunk_w2": bell_draw(splits[8], (HIDDEN_SIZE, LATENT), HIDDEN_SIZE ** -0.5, 0.1875),
        "trunk_b2": bell_draw(splits[9], (LATENT,), 0.5, 3.0, (), jnp.float32),
    }


def reference(sensors, branch_w, branch_b, coords, func_index, targets, trunk_w1, trunk_b1, trunk_w2, trunk_b2):
    pre = jnp.einsum('kfs,ksl->kfl', sensors.astype(jnp.float32), branch_w.astype(jnp.float32)) + branch_b[:, None, :]
    latent = jnp.tanh(pre).astype(jnp.bfloat16)
    lat_full = latent.astype(jnp.float32)
    product = (lat_full[0] * lat_full[1] * lat_full[2]).astype(jnp.bfloat16)
    prod_full = product.astype(jnp.float32)
    scale = LATENT ** -0.5
    blocks = QUERIES // QRY_DEV
    coord_blocks = coords.reshape(DIMS, blocks, QRY_DEV).transpose(1, 0, 2)
    index_blocks = func_index.reshape(blocks, QRY_DEV)
    target_blocks = targets.reshape(blocks, QRY_DEV)

    def visit(carry, item):
        gw1, gb1, gw2, gb2, dprod = carry
        number, cblock, iblock, tblock = item
        owner = (iblock + (number // N_QUERY) * GROUP_FUNCS).astype(jnp.int32)
        first = lax.dot_general(cblock, trunk_w1, (((0,), (0,)), ((), ())), preferred_element_type=jnp.float32)
        hidden = jnp.tanh(first + trunk_b1).astype(jnp.bfloat16)
        trunk_out = jnp.dot(hidden, trunk_w2, preferred_element_type=jnp.float32) + trunk_b2
        picked = jnp.take(prod_full, owner, axis=0)
        pred = jnp.sum(picked * trunk_out, axis=1) * scale
        resid = (pred - tblock) / FUNCS
        weighted = (resid[:, None] * trunk_out * scale).astype(jnp.bfloat16)
        dprod = dprod + jax.ops.segment_sum(weighted.astype(jnp.float32), owner, FUNCS)
        grad_out = (resid[:, None] * picked * scale).astype(jnp.bfloat16)
        gw2 = gw2 + lax.dot_general(hidden, grad_out, (((0,), (0,)), ((), ())), preferred_element_type=jnp.float32)
        gb2 = gb2 + jnp.sum(grad_out.astype(jnp.float32), axis=0)
        grad_hidden = lax.dot_general(grad_out, trunk_w2, (((1,), (1,)), ((), ())), preferred_element_type=jnp.float32)
        hid_full = hidden.astype(jnp.float32)
        grad_pre = (grad_hidden * (1.0 - hid_full * hid_full)).astype(jnp.bfloat16)
        gw1 = gw1 + lax.dot_general(cblock, grad_pre, (((1,), (0,)), ((), ())), preferred_element_type=jnp.float32)
        gb1 = gb1 + jnp.sum(grad_pre.astype(jnp.float32), axis=0)
        return (gw1, gb1, gw2, gb2, dprod), None

    start = (jnp.zeros((DIMS, HIDDEN_SIZE), jnp.float32), jnp.zeros((HIDDEN_SIZE,), jnp.float32),
             jnp.zeros((HIDDEN_SIZE, LATENT), jnp.float32), jnp.zeros((LATENT,), jnp.float32),
             jnp.zeros((FUNCS, LATENT), jnp.float32))
    numbers = jnp.arange(blocks, dtype=jnp.int32)
    (gw1, gb1, gw2, gb2, dprod), _ = lax.scan(visit, start, (numbers, coord_blocks, index_blocks, target_blocks))
    others = jnp.stack([lat_full[1] * lat_full[2], lat_full[0] * lat_full[2], lat_full[0] * lat_full[1]])
    delta = (dprod[None] * others * (1.0 - lat_full * lat_full)).astype(jnp.bfloat16)
    delta_full = delta.astype(jnp.float32)
    grad_branch_w = jnp.einsum('kfs,kfl->ksl', sensors.astype(jnp.float32), delta_full)
    grad_branch_b = jnp.sum(delta_full, axis=1)
    return grad_branch_w, grad_branch_b, gw1, gb1, gw2, gb2
```

```python
import functools

import jax
import jax.numpy as jnp
from jax import lax
from jax.experimental import pallas as pl
from jax.experimental.pallas import tpu as pltpu
from jax.sharding import PartitionSpec as P

F32 = jnp.float32
BF16 = jnp.bfloat16
ROWS = 12
CHUNKS = 4
VMEM = pltpu.VMEM


def nt(a, b):
    return lax.dot_general(a, b, (((1,), (1,)), ((), ())), preferred_element_type=F32)


def tn(a, b):
    return lax.dot_general(a, b, (((0,), (0,)), ((), ())), preferred_element_type=F32)


def nn(a, b):
    return lax.dot_general(a, b, (((1,), (0,)), ((), ())), preferred_element_type=F32)


def split(x):
    high = x.astype(BF16)
    return high, (x - high.astype(F32)).astype(BF16)


def exchange_kernel(
    sens, bw, bb, coords, fidx, targ, w1, b1, w2, b2,
    hm_out, p_out, d_out, sg_out, s_out, g_out,
    wbuf, w2buf, row8, prodsend, prodbuf, pf, latbuf, lf, sensend, sgbuf, sgf,
    hid, omh, msgf, msg, rsbuf, agbuf, hf,
    wsem, w2sem, psend, precv, lsend, lrecv, ssend, srecv, rsend, rrecv, asend, arecv,
    dsend, drecv,
):
    branch = lax.axis_index("branch")
    q = lax.axis_index("query")
    core = lax.rem(branch, 2)
    zlo = lax.div(branch, 2)
    zhi, xy = lax.div(q, 16), lax.rem(q, 16)
    x, y = lax.div(xy, 4), lax.rem(xy, 4)
    scale = 1.0 / 32.0
    rows = bw.shape[1] // CHUNKS

    def peer(d):
        dl, dq = lax.div(d, 32), lax.rem(d, 32)
        dh, dx, dy = lax.div(dq, 16), lax.rem(lax.div(dq, 4), 4), lax.rem(dq, 4)
        pz = lax.rem(zlo + dl, 2)
        pq = lax.rem(zhi + dh, 2) * 16 + lax.rem(x + dx, 4) * 4 + lax.rem(y + dy, 4)
        return pz * 2 + core, pq

    partner = (zlo * 2 + (1 - core), q)
    mine = core * 64 + zlo * 32 + q

    def wcopy(k, c):
        part = pl.ds(c * rows, rows)
        return pltpu.make_async_copy(bw.at[k, part], wbuf.at[k, part], wsem.at[k, c])

    for k in range(3):
        for c in range(CHUNKS):
            wcopy(k, c).start()
    w2copy = pltpu.make_async_copy(w2, w2buf, w2sem)
    w2copy.start()

    barrier = pltpu.get_barrier_semaphore()

    def greet(i, carry):
        pl.semaphore_signal(barrier, inc=1, device_id=peer(i), device_id_type=pl.DeviceIdType.MESH)
        return carry

    lax.fori_loop(1, 64, greet, 0)
    pl.semaphore_signal(barrier, inc=1, device_id=partner, device_id_type=pl.DeviceIdType.MESH)

    def to_peers(lo, hi, source, target, send, recv):
        def one(i, carry):
            d = hi - 1 - i
            device = peer(d)
            pltpu.make_async_remote_copy(
                src_ref=source(device), dst_ref=target(device), send_sem=send, recv_sem=recv,
                device_id=device, device_id_type=pl.DeviceIdType.MESH,
            ).start()
            return carry

        lax.fori_loop(0, hi - lo, one, 0)

    def wait(ref, sem):
        pltpu.make_async_copy(ref, ref, sem).wait()

    def swap(buf, i):
        half = buf.at[pl.ds(core * 64, 64)]
        return pltpu.make_async_remote_copy(
            src_ref=half, dst_ref=half, send_sem=dsend.at[i], recv_sem=drecv.at[i],
            device_id=partner, device_id_type=pl.DeviceIdType.MESH,
        )

    for k in range(3):
        sk = sens[k].astype(F32)
        for j in range(16):
            sgf[4 * j + k : 4 * j + k + 1, :] = sk[:, 128 * j : 128 * (j + 1)]
    for j in range(16):
        sensend[j] = sgf[4 * j : 4 * j + 4, :].astype(BF16)

    lats = []
    for k in range(3):
        pre = bb[k : k + 1, :]
        for c in range(CHUNKS):
            wcopy(k, c).wait()
            pre = pre + nn(sens[k][:, c * rows : (c + 1) * rows], wbuf[k, c * rows : (c + 1) * rows, :])
        lat = jnp.tanh(pre).astype(BF16).astype(F32)
        lats.append(lat)
        for j in range(8):
            row8[k, j : j + 1, :] = lat[:, 128 * j : 128 * (j + 1)]
        latbuf[mine, k] = row8[k].astype(BF16)
    own = (row8[0] * row8[1] * row8[2]).astype(BF16)
    prodsend[...] = own
    prodbuf[q] = own

    pl.semaphore_wait(barrier, 64)

    to_peers(1, 32, lambda d: prodsend, lambda d: prodbuf.at[q], psend, precv)
    to_peers(1, 64, lambda d: latbuf.at[mine], lambda d: latbuf.at[mine], lsend, lrecv)
    to_peers(1, 64, lambda d: sensend.at[lax.div(d[1], 2)], lambda d: sgbuf.at[mine], ssend, srecv)
    sgbuf[mine] = sensend[lax.div(q, 2)]

    for r in range(4):
        part = slice(128 * r, 128 * (r + 1))
        h = jnp.tanh(tn(coords[:, part], w1[...]) + b1[...]).astype(BF16)
        hid[part, :] = h
        hw = h.astype(F32)
        omh[part, :] = (1.0 - hw * hw).astype(BF16)

    owned = lax.broadcasted_iota(jnp.int32, (32, 512), 0) == fidx[...]

    w2copy.wait()
    wait(prodbuf.at[pl.ds(0, 31)], precv)
    for f in range(32):
        pf[8 * f : 8 * f + 8, :] = prodbuf[f].astype(F32)
    prod = jnp.concatenate([pf[pl.ds(j, 32, stride=8), :] for j in range(8)], axis=1)
    shift = jnp.sum(prod * b2[...], axis=1, keepdims=True)
    quad = nt(prod.astype(BF16), w2buf[...])
    qh, ql = split(quad)
    dots = nt(jnp.concatenate([qh, ql], axis=0), hid[...])
    dots = dots[:32] + dots[32:] + shift
    pred = jnp.sum(jnp.where(owned, dots, 0.0), axis=0, keepdims=True) * scale
    resid = (pred - targ[...]) * (1.0 / 128.0)
    a = jnp.where(owned, resid * scale, 0.0)
    ah, al = split(a)
    hsum = nn(jnp.concatenate([ah, al], axis=0), hid[...])
    hsum = hsum[:32] + hsum[32:]
    asum = jnp.sum(a, axis=1, keepdims=True)
    cf = coords[...].astype(F32)
    za = jnp.concatenate([a * cf[c : c + 1, :] for c in range(3)] + [a], axis=0).astype(BF16)
    z = nn(za, omh[...])
    gw1 = [jnp.sum(quad * z[32 * c : 32 * c + 32, :], axis=0, keepdims=True) for c in range(4)]
    for j in range(8):
        msgf[pl.ds(j, 32, stride=16), :] = hsum[:, 128 * j : 128 * (j + 1)]
        for c in range(4):
            at = 16 * (8 * c + j) + 8
            msgf[at : at + 1, :] = gw1[c][:, 128 * j : 128 * (j + 1)]
    sh, sl = split(asum)
    msgf[pl.ds(9, 32, stride=16), :] = jnp.broadcast_to(sh.astype(F32), (32, 128))
    msgf[pl.ds(10, 32, stride=16), :] = jnp.broadcast_to(sl.astype(F32), (32, 128))
    msgf[pl.ds(11, 32, stride=16), :] = jnp.zeros((32, 128), F32)
    for f in range(32):
        msg[f] = msgf[16 * f : 16 * f + ROWS, :].astype(BF16)

    to_peers(1, 32, lambda d: msg.at[d[1]], lambda d: rsbuf.at[q], rsend, rrecv)
    rsbuf[q] = msg[q]

    wait(latbuf.at[pl.ds(0, 63)], lrecv)
    wait(sgbuf.at[pl.ds(0, 63)], srecv)
    swap_lat, swap_sens = swap(latbuf, 0), swap(sgbuf, 1)
    swap_lat.start()
    swap_sens.start()

    wait(rsbuf.at[pl.ds(0, 31)], rrecv)
    total = rsbuf[0].astype(F32)
    for f in range(1, 32):
        total = total + rsbuf[f].astype(F32)
    hf[0:ROWS, :] = total
    s = hf[9:10, :] + hf[10:11, :]
    sh = s.astype(BF16).astype(F32)
    hf[9:10, :] = sh
    hf[10:11, :] = s - sh
    agbuf[mine] = hf[0:ROWS, :].astype(BF16)
    to_peers(1, 64, lambda d: agbuf.at[mine], lambda d: agbuf.at[mine], asend, arecv)

    swap_lat.wait()
    swap_sens.wait()

    def spread(i, carry):
        at = pl.multiple_of(i * 8, 8)
        for k in range(3):
            lf[k, pl.ds(at, 8), :] = latbuf[i, k].astype(F32)
        return carry

    lax.fori_loop(0, 128, spread, 0, unroll=4)

    def spread_sens(i, carry):
        sgf[pl.ds(i * 4, 4), :] = sgbuf[i].astype(F32)
        return carry

    lax.fori_loop(0, 128, spread_sens, 0, unroll=4)
    odd = lax.rem(q, 2) == 1
    for k in range(3):
        cols = sgf[pl.ds(k, 128, stride=4), :]
        sg_out[k] = jnp.where(odd, pltpu.roll(cols, 64, 1), cols).astype(BF16)
    for j in range(8):
        l0, l1, l2 = [lf[k, pl.ds(j, 128, stride=8), :] for k in range(3)]
        cols = slice(128 * j, 128 * (j + 1))
        m12, m02, m01 = l1 * l2, l0 * l2, l0 * l1
        p_out[:, cols] = (m01 * l2).astype(BF16)
        d_out[0, :, cols] = m12 * (1.0 - l0 * l0)
        d_out[1, :, cols] = m02 * (1.0 - l1 * l1)
        d_out[2, :, cols] = m01 * (1.0 - l2 * l2)

    wait(agbuf.at[pl.ds(0, 63)], arecv)
    swap_h = swap(agbuf, 2)
    swap_h.start()
    wait(prodbuf.at[pl.ds(0, 31)], psend)
    wait(latbuf.at[pl.ds(0, 63)], lsend)
    wait(sgbuf.at[pl.ds(0, 63)], ssend)
    wait(rsbuf.at[pl.ds(0, 31)], rsend)
    wait(agbuf.at[pl.ds(0, 63)], asend)
    swap_h.wait()

    def spread_h(i, carry):
        at = pl.multiple_of(i * 16, 16)
        hf[pl.ds(at, ROWS), :] = agbuf[i].astype(F32)
        return carry

    lax.fori_loop(0, 128, spread_h, 0, unroll=4)
    for j in range(8):
        hm_out[:, 128 * j : 128 * (j + 1)] = hf[pl.ds(j, 128, stride=16), :].astype(BF16)
    s_out[...] = hf[pl.ds(9, 128, stride=16), :] + hf[pl.ds(10, 128, stride=16), :]
    g = hf[pl.ds(8, 128, stride=16), :]
    g_out[...] = (g[0:32] + g[32:64]) + (g[64:96] + g[96:128])


def output_kernel(
    hm, prod, d, sg, s, g, w2, b2,
    gbw_out, gbb_out, gw1_out, gb1_out, gw2_out, gb2_out, gw2buf, sem,
):
    def drain(c):
        part = pl.ds(256 * c, 256)
        return pltpu.make_async_copy(gw2buf.at[part], gw2_out.at[part], sem.at[c])

    for c in range(4):
        gw2buf[256 * c : 256 * (c + 1), :] = tn(hm[:, 256 * c : 256 * (c + 1)], prod[...])
        drain(c).start()
    sums = s[:, 0:1]
    gp = nn(hm[...], w2[...]) + sums * b2[...]
    for k in range(3):
        delta = (gp * d[k]).astype(BF16)
        gbw_out[k] = tn(sg[k], delta)[0:64, :]
        gbb_out[k : k + 1, :] = jnp.sum(delta.astype(F32), axis=0, keepdims=True)
    gb2_out[...] = jnp.sum(sums * prod[...].astype(F32), axis=0, keepdims=True)
    for j in range(8):
        cols = slice(128 * j, 128 * (j + 1))
        for c in range(3):
            gw1_out[c : c + 1, cols] = g[8 * c + j : 8 * c + j + 1, :]
        gb1_out[:, cols] = g[24 + j : 25 + j, :]
    for c in range(4):
        drain(c).wait()


def shards(sensors, branch_w, branch_b, coords, func_index, targets, trunk_w1, trunk_b1, trunk_w2, trunk_b2):
    vmem = pl.BlockSpec(memory_space=pltpu.VMEM)
    hbm = pl.BlockSpec(memory_space=pl.ANY)
    b2 = trunk_b2.reshape(1, 1024)
    shape = jax.ShapeDtypeStruct
    dma = pltpu.SemaphoreType.DMA
    hm, prod, d, sg, s, g = pl.pallas_call(
        exchange_kernel,
        out_shape=(
            shape((128, 1024), BF16), shape((128, 1024), BF16), shape((3, 128, 1024), F32),
            shape((3, 128, 128), BF16), shape((128, 128), F32), shape((32, 128), F32),
        ),
        in_specs=[vmem, hbm, vmem, vmem, vmem, vmem, vmem, vmem, hbm, vmem],
        out_specs=(vmem,) * 6,
        scratch_shapes=[
            VMEM((3, 2048, 1024), BF16), VMEM((1024, 1024), BF16), VMEM((3, 8, 128), F32),
            VMEM((8, 128), BF16), VMEM((32, 8, 128), BF16), VMEM((256, 128), F32),
            VMEM((128, 3, 8, 128), BF16), VMEM((3, 1024, 128), F32),
            VMEM((16, 4, 128), BF16), VMEM((128, 4, 128), BF16), VMEM((512, 128), F32),
            VMEM((512, 1024), BF16), VMEM((512, 1024), BF16),
            VMEM((512, 128), F32), VMEM((32, ROWS, 128), BF16), VMEM((32, ROWS, 128), BF16),
            VMEM((128, ROWS, 128), BF16), VMEM((2048, 128), F32),
            dma((3, CHUNKS)), dma, dma, dma, dma, dma, dma, dma, dma, dma, dma, dma,
            dma((3,)), dma((3,)),
        ],
        compiler_params=pltpu.CompilerParams(
            collective_id=0, has_side_effects=True, vmem_limit_bytes=40 * 1024 * 1024
        ),
        name="exchange",
    )(
        sensors, branch_w, branch_b, coords, func_index.reshape(1, 512), targets.reshape(1, 512),
        trunk_w1, trunk_b1.reshape(1, 1024), trunk_w2, b2,
    )
    gbw, gbb, gw1, gb1, gw2, gb2 = pl.pallas_call(
        output_kernel,
        out_shape=(
            shape((3, 64, 1024), F32), shape((3, 1024), F32), shape((3, 1024), F32),
            shape((1, 1024), F32), shape((1024, 1024), F32), shape((1, 1024), F32),
        ),
        in_specs=[vmem] * 8,
        out_specs=(vmem, vmem, vmem, vmem, hbm, vmem),
        scratch_shapes=[VMEM((1024, 1024), F32), dma((4,))],
        compiler_params=pltpu.CompilerParams(vmem_limit_bytes=32 * 1024 * 1024),
        name="outputs",
    )(hm, prod, d, sg, s, g, trunk_w2, b2)
    return gbw, gbb, gw1, gb1.reshape(1024), gw2, gb2.reshape(1024)


def solution(mesh):
    both = ("branch", "query")
    placed = (P(None, both, None), P(), P(), P(None, both), P(both), P(both), P(), P(), P(), P())
    return jax.shard_map(
        shards,
        mesh=mesh,
        in_specs=placed,
        out_specs=(P(None, "query", None), P(), P(), P(), P(), P()),
        check_vma=False,
    )
```

```python
import jax
import jax.numpy as jnp
from jax import lax
from jax.experimental import pallas as pl
from jax.experimental.pallas import tpu as pltpu
from jax.sharding import PartitionSpec as P

F32 = jnp.float32
BF16 = jnp.bfloat16
ROWS = 12
CHUNKS = 4
VMEM = pltpu.VMEM


def nt(a, b):
    return lax.dot_general(a, b, (((1,), (1,)), ((), ())), preferred_element_type=F32)


def tn(a, b):
    return lax.dot_general(a, b, (((0,), (0,)), ((), ())), preferred_element_type=F32)


def nn(a, b):
    return lax.dot_general(a, b, (((1,), (0,)), ((), ())), preferred_element_type=F32)


def split(x):
    high = x.astype(BF16)
    return high, (x - high.astype(F32)).astype(BF16)


def exchange_kernel(
    sens_hbm, bw, bb_hbm, coords_hbm, fidx_hbm, targ_hbm, w1_hbm, b1_hbm, w2, b2_hbm,
    hm_out, p_out, delta_out, sg_out, s_out, g_out,
    sens, bb, coords, fidx, targ, w1, b1, b2, d_scr,
    wbuf, w2buf, row8, prodsend, prodbuf, pf, latbuf, lf, sensend, sgbuf, sgf,
    hid, omh, msgf, msg, rsbuf, agbuf, hf,
    insem, wsem, w2sem, psend, precv, lsend, lrecv, ssend, srecv, rsend, rrecv, asend, arecv,
    dsend, drecv,
):
    branch = lax.axis_index("branch")
    q = lax.axis_index("query")
    core = lax.rem(branch, 2)
    zlo = lax.div(branch, 2)
    zhi, xy = lax.div(q, 16), lax.rem(q, 16)
    x, y = lax.div(xy, 4), lax.rem(xy, 4)
    scale = 1.0 / 32.0
    rows = bw.shape[1] // CHUNKS

    def far(t):
        return t + lax.div(t, 2) - 2 * lax.div(t, 3)

    def peer(d):
        dl, dq = lax.div(d, 32), lax.rem(d, 32)
        dh, dx, dy = lax.div(dq, 16), far(lax.rem(lax.div(dq, 4), 4)), far(lax.rem(dq, 4))
        pz = lax.rem(zlo + dl, 2)
        pq = lax.rem(zhi + dh, 2) * 16 + lax.rem(x + dx, 4) * 4 + lax.rem(y + dy, 4)
        return pz * 2 + core, pq

    partner = (zlo * 2 + (1 - core), q)
    mine = core * 64 + zlo * 32 + q

    def wcopy(k, c):
        part = pl.ds(c * rows, rows)
        return pltpu.make_async_copy(bw.at[k, part], wbuf.at[k, part], wsem.at[k, c])

    smalls = ((sens_hbm, sens), (bb_hbm, bb), (coords_hbm, coords), (w1_hbm, w1), (b1_hbm, b1),
              (fidx_hbm, fidx), (targ_hbm, targ), (b2_hbm, b2))
    loads = [pltpu.make_async_copy(a, b, insem.at[i]) for i, (a, b) in enumerate(smalls)]
    loads[0].start()
    wcopy(0, 0).start()
    for load in loads[1:]:
        load.start()
    for k in range(3):
        for c in range(CHUNKS):
            if k + c:
                wcopy(k, c).start()
    w2copy = pltpu.make_async_copy(w2, w2buf, w2sem)
    w2copy.start()

    barrier = pltpu.get_barrier_semaphore()

    def greet(i, carry):
        pl.semaphore_signal(barrier, inc=1, device_id=peer(i), device_id_type=pl.DeviceIdType.MESH)
        return carry

    lax.fori_loop(1, 64, greet, 0)
    pl.semaphore_signal(barrier, inc=1, device_id=partner, device_id_type=pl.DeviceIdType.MESH)

    def to_peers(lo, hi, source, target, send, recv):
        def one(i, carry):
            d = hi - 1 - i
            device = peer(d)
            pltpu.make_async_remote_copy(
                src_ref=source(device), dst_ref=target(device), send_sem=send, recv_sem=recv,
                device_id=device, device_id_type=pl.DeviceIdType.MESH,
            ).start()
            return carry

        lax.fori_loop(0, hi - lo, one, 0)

    def wait(ref, sem):
        pltpu.make_async_copy(ref, ref, sem).wait()

    def swap(buf, i):
        half = buf.at[pl.ds(core * 64, 64)]
        return pltpu.make_async_remote_copy(
            src_ref=half, dst_ref=half, send_sem=dsend.at[i], recv_sem=drecv.at[i],
            device_id=partner, device_id_type=pl.DeviceIdType.MESH,
        )

    loads[0].wait()
    for k in range(3):
        sk = sens[k : k + 1, :].astype(F32)
        for j in range(16):
            sgf[4 * j + k : 4 * j + k + 1, :] = sk[:, 128 * j : 128 * (j + 1)]
    for j in range(16):
        sensend[j] = sgf[4 * j : 4 * j + 4, :].astype(BF16)

    loads[1].wait()
    for k in range(3):
        pre = bb[k : k + 1, :]
        for c in range(CHUNKS):
            wcopy(k, c).wait()
            pre = pre + nn(sens[k : k + 1, c * rows : (c + 1) * rows], wbuf[k, c * rows : (c + 1) * rows, :])
        lat = jnp.tanh(pre).astype(BF16).astype(F32)
        for j in range(8):
            row8[k, j : j + 1, :] = lat[:, 128 * j : 128 * (j + 1)]
        latbuf[mine, k] = row8[k].astype(BF16)
    own = (row8[0] * row8[1] * row8[2]).astype(BF16)
    prodsend[...] = own
    prodbuf[q] = own

    pl.semaphore_wait(barrier, 64)

    to_peers(1, 32, lambda d: prodsend, lambda d: prodbuf.at[q], psend, precv)
    to_peers(1, 64, lambda d: latbuf.at[mine], lambda d: latbuf.at[mine], lsend, lrecv)
    to_peers(1, 64, lambda d: sensend.at[lax.div(d[1], 2)], lambda d: sgbuf.at[mine], ssend, srecv)
    sgbuf[mine] = sensend[lax.div(q, 2)]

    for load in loads[2:]:
        load.wait()
    for r in range(4):
        part = slice(128 * r, 128 * (r + 1))
        h = jnp.tanh(tn(coords[:, part], w1[...]) + b1[...]).astype(BF16)
        hid[part, :] = h
        hw = h.astype(F32)
        omh[part, :] = (1.0 - hw * hw).astype(BF16)

    owned = lax.broadcasted_iota(jnp.int32, (32, 512), 0) == fidx[...]

    w2copy.wait()
    wait(prodbuf.at[pl.ds(0, 31)], precv)
    for f in range(32):
        pf[8 * f : 8 * f + 8, :] = prodbuf[f].astype(F32)
    prod = jnp.concatenate([pf[pl.ds(j, 32, stride=8), :] for j in range(8)], axis=1)
    shift = jnp.sum(prod * b2[...], axis=1, keepdims=True)
    quad = nt(prod.astype(BF16), w2buf[...])
    qh, ql = split(quad)
    dots = nt(jnp.concatenate([qh, ql], axis=0), hid[...])
    dots = dots[:32] + dots[32:] + shift
    pred = jnp.sum(jnp.where(owned, dots, 0.0), axis=0, keepdims=True) * scale
    resid = (pred - targ[...]) * (1.0 / 128.0)
    a = jnp.where(owned, resid * scale, 0.0)
    ah, al = split(a)
    hsum = nn(jnp.concatenate([ah, al], axis=0), hid[...])
    hsum = hsum[:32] + hsum[32:]
    asum = jnp.sum(a, axis=1, keepdims=True)
    cf = coords[...].astype(F32)
    za = jnp.concatenate([a * cf[c : c + 1, :] for c in range(3)] + [a], axis=0).astype(BF16)
    z = nn(za, omh[...])
    gw1 = [jnp.sum(quad * z[32 * c : 32 * c + 32, :], axis=0, keepdims=True) for c in range(4)]
    for j in range(8):
        msgf[pl.ds(j, 32, stride=16), :] = hsum[:, 128 * j : 128 * (j + 1)]
        for c in range(4):
            at = 16 * (8 * c + j) + 8
            msgf[at : at + 1, :] = gw1[c][:, 128 * j : 128 * (j + 1)]
    sh, sl = split(asum)
    msgf[pl.ds(9, 32, stride=16), :] = jnp.broadcast_to(sh.astype(F32), (32, 128))
    msgf[pl.ds(10, 32, stride=16), :] = jnp.broadcast_to(sl.astype(F32), (32, 128))
    msgf[pl.ds(11, 32, stride=16), :] = jnp.zeros((32, 128), F32)
    for f in range(32):
        msg[f] = msgf[16 * f : 16 * f + ROWS, :].astype(BF16)

    to_peers(1, 32, lambda d: msg.at[d[1]], lambda d: rsbuf.at[q], rsend, rrecv)
    rsbuf[q] = msg[q]

    wait(latbuf.at[pl.ds(0, 63)], lrecv)
    wait(sgbuf.at[pl.ds(0, 63)], srecv)
    swap_lat, swap_sens = swap(latbuf, 0), swap(sgbuf, 1)
    swap_lat.start()
    swap_sens.start()

    wait(rsbuf.at[pl.ds(0, 31)], rrecv)
    total = rsbuf[0].astype(F32)
    for f in range(1, 32):
        total = total + rsbuf[f].astype(F32)
    hf[0:ROWS, :] = total
    s = hf[9:10, :] + hf[10:11, :]
    sh = s.astype(BF16).astype(F32)
    hf[9:10, :] = sh
    hf[10:11, :] = s - sh
    agbuf[mine] = hf[0:ROWS, :].astype(BF16)
    to_peers(1, 64, lambda d: agbuf.at[mine], lambda d: agbuf.at[mine], asend, arecv)

    swap_lat.wait()
    swap_sens.wait()

    def spread(i, carry):
        at = pl.multiple_of(i * 8, 8)
        for k in range(3):
            lf[k, pl.ds(at, 8), :] = latbuf[i, k].astype(F32)
        return carry

    lax.fori_loop(0, 128, spread, 0, unroll=4)

    def spread_sens(i, carry):
        sgf[pl.ds(i * 4, 4), :] = sgbuf[i].astype(F32)
        return carry

    lax.fori_loop(0, 128, spread_sens, 0, unroll=4)
    odd = lax.rem(q, 2) == 1
    for k in range(3):
        cols = sgf[pl.ds(k, 128, stride=4), :]
        sg_out[k] = jnp.where(odd, pltpu.roll(cols, 64, 1), cols).astype(BF16)
    for j in range(8):
        l0, l1, l2 = [lf[k, pl.ds(j, 128, stride=8), :] for k in range(3)]
        cols = slice(128 * j, 128 * (j + 1))
        m12, m02, m01 = l1 * l2, l0 * l2, l0 * l1
        p_out[:, cols] = (m01 * l2).astype(BF16)
        d_scr[0, :, cols] = m12 * (1.0 - l0 * l0)
        d_scr[1, :, cols] = m02 * (1.0 - l1 * l1)
        d_scr[2, :, cols] = m01 * (1.0 - l2 * l2)

    wait(agbuf.at[pl.ds(0, 63)], arecv)
    swap_h = swap(agbuf, 2)
    swap_h.start()

    def finish(half):
        base = pl.multiple_of(half * 64, 64)

        def spread_h(i, carry):
            at = pl.multiple_of(i * 16, 16)
            hf[pl.ds(at, ROWS), :] = agbuf[base + i].astype(F32)
            return carry

        lax.fori_loop(0, 64, spread_h, 0, unroll=4)
        hm = jnp.concatenate([hf[pl.ds(j, 64, stride=16), :].astype(BF16) for j in range(8)], axis=1)
        sums = hf[pl.ds(9, 64, stride=16), :] + hf[pl.ds(10, 64, stride=16), :]
        g = hf[pl.ds(8, 64, stride=16), :]
        here = pl.ds(base, 64)
        hm_out[here, :] = hm
        s_out[here, :] = sums
        gp = nn(hm, w2buf[...]) + sums[:, 0:1] * b2[...]
        for k in range(3):
            delta_out[k, here, :] = (gp * d_scr[k, here, :]).astype(BF16)
        return g[0:32] + g[32:64]

    g_own = finish(core)
    wait(prodbuf.at[pl.ds(0, 31)], psend)
    wait(latbuf.at[pl.ds(0, 63)], lsend)
    wait(sgbuf.at[pl.ds(0, 63)], ssend)
    wait(rsbuf.at[pl.ds(0, 31)], rsend)
    wait(agbuf.at[pl.ds(0, 63)], asend)
    swap_h.wait()
    g_out[...] = g_own + finish(1 - core)


def output_kernel(
    hm, prod, delta, sg, s, g,
    gbw_out, gbb_out, gw1_out, gb1_out, gw2_out, gb2_out,
    gbw, gbb, gw1, gb1, gw2, gb2, sem,
):
    copies = []

    def drain(source, target):
        copies.append(pltpu.make_async_copy(source, target, sem.at[len(copies)]))
        copies[-1].start()

    for c in range(4):
        part = pl.ds(256 * c, 256)
        gw2[256 * c : 256 * (c + 1), :] = tn(hm[:, 256 * c : 256 * (c + 1)], prod[...])
        drain(gw2.at[part], gw2_out.at[part])
    for k in range(3):
        gbw[k] = tn(sg[k], delta[k])[0:64, :]
        drain(gbw.at[k], gbw_out.at[k])
    for k in range(3):
        gbb[k : k + 1, :] = jnp.sum(delta[k].astype(F32), axis=0, keepdims=True)
    gb2[...] = jnp.sum(s[:, 0:1] * prod[...].astype(F32), axis=0, keepdims=True)
    for j in range(8):
        cols = slice(128 * j, 128 * (j + 1))
        for c in range(3):
            gw1[c : c + 1, cols] = g[8 * c + j : 8 * c + j + 1, :]
        gb1[:, cols] = g[24 + j : 25 + j, :]
    drain(gbb, gbb_out)
    drain(gb2, gb2_out)
    drain(gw1, gw1_out)
    drain(gb1, gb1_out)
    for copy in copies:
        copy.wait()


def shards(sensors, branch_w, branch_b, coords, func_index, targets, trunk_w1, trunk_b1, trunk_w2, trunk_b2):
    vmem = pl.BlockSpec(memory_space=pltpu.VMEM)
    hbm = pl.BlockSpec(memory_space=pltpu.HBM)
    shape = jax.ShapeDtypeStruct
    dma = pltpu.SemaphoreType.DMA
    inputs = (
        sensors.reshape(3, 2048), branch_w, branch_b, coords, func_index.reshape(1, 512),
        targets.reshape(1, 512), trunk_w1, trunk_b1.reshape(1, 1024), trunk_w2, trunk_b2.reshape(1, 1024),
    )
    passed = pl.pallas_call(
        exchange_kernel,
        out_shape=(
            shape((128, 1024), BF16), shape((128, 1024), BF16), shape((3, 128, 1024), BF16),
            shape((3, 128, 128), BF16), shape((128, 128), F32), shape((32, 128), F32),
        ),
        in_specs=[hbm] * 10,
        out_specs=(vmem,) * 6,
        scratch_shapes=[
            VMEM((3, 2048), BF16), VMEM((3, 1024), F32), VMEM((3, 512), BF16), VMEM((1, 512), jnp.int32),
            VMEM((1, 512), F32), VMEM((3, 1024), BF16), VMEM((1, 1024), F32), VMEM((1, 1024), F32),
            VMEM((3, 128, 1024), F32),
            VMEM((3, 2048, 1024), BF16), VMEM((1024, 1024), BF16), VMEM((3, 8, 128), F32),
            VMEM((8, 128), BF16), VMEM((32, 8, 128), BF16), VMEM((256, 128), F32),
            VMEM((128, 3, 8, 128), BF16), VMEM((3, 1024, 128), F32),
            VMEM((16, 4, 128), BF16), VMEM((128, 4, 128), BF16), VMEM((512, 128), F32),
            VMEM((512, 1024), BF16), VMEM((512, 1024), BF16),
            VMEM((512, 128), F32), VMEM((32, ROWS, 128), BF16), VMEM((32, ROWS, 128), BF16),
            VMEM((128, ROWS, 128), BF16), VMEM((1024, 128), F32),
            dma((8,)), dma((3, CHUNKS)), dma, dma, dma, dma, dma, dma, dma, dma, dma, dma, dma,
            dma((3,)), dma((3,)),
        ],
        compiler_params=pltpu.CompilerParams(
            collective_id=0, has_side_effects=True, vmem_limit_bytes=40 * 1024 * 1024
        ),
        name="exchange",
    )(*[pltpu.with_memory_space_constraint(v, pltpu.HBM) for v in inputs])
    results = (
        shape((3, 64, 1024), F32), shape((3, 1024), F32), shape((3, 1024), F32),
        shape((1, 1024), F32), shape((1024, 1024), F32), shape((1, 1024), F32),
    )
    gbw, gbb, gw1, gb1, gw2, gb2 = pl.pallas_call(
        output_kernel,
        out_shape=results,
        in_specs=[vmem] * 6,
        out_specs=(hbm,) * 6,
        scratch_shapes=[VMEM(r.shape, F32) for r in results] + [dma((11,))],
        compiler_params=pltpu.CompilerParams(vmem_limit_bytes=16 * 1024 * 1024),
        name="outputs",
    )(*passed)
    return gbw, gbb, gw1, gb1.reshape(1024), gw2, gb2.reshape(1024)


def solution(mesh):
    both = ("branch", "query")
    placed = (P(None, both, None), P(), P(), P(None, both), P(both), P(both), P(), P(), P(), P())
    return jax.shard_map(
        shards,
        mesh=mesh,
        in_specs=placed,
        out_specs=(P(None, "query", None), P(), P(), P(), P(), P()),
        check_vma=False,
    )
```

```python
import jax
import jax.numpy as jnp
from jax import lax
from jax.experimental import pallas as pl
from jax.experimental.pallas import tpu as pltpu
from jax.sharding import PartitionSpec as P

F32 = jnp.float32
BF16 = jnp.bfloat16
ROWS = 12
CHUNKS = 4
VMEM = pltpu.VMEM


def nt(a, b):
    return lax.dot_general(a, b, (((1,), (1,)), ((), ())), preferred_element_type=F32)


def tn(a, b):
    return lax.dot_general(a, b, (((0,), (0,)), ((), ())), preferred_element_type=F32)


def nn(a, b):
    return lax.dot_general(a, b, (((1,), (0,)), ((), ())), preferred_element_type=F32)


def split(x):
    high = x.astype(BF16)
    return high, (x - high.astype(F32)).astype(BF16)


def exchange_kernel(
    sens_hbm, bw, bb_hbm, coords_hbm, fidx_hbm, targ_hbm, w1_hbm, b1_hbm, w2, b2_hbm,
    hm_out, p_out, delta_out, sg_out, s_out, g_out,
    sens, bb, coords, fidx, targ, w1, b1, b2, d_scr,
    wbuf, w2buf, row8, prodsend, prodbuf, pf, latbuf, lf, sensend, sgbuf, sgf,
    hid, omh, msgf, msg, rsbuf, agbuf, hf,
    insem, wsem, w2sem, psend, precv, lsend, lrecv, ssend, srecv, rsend, rrecv, asend, arecv,
    dsend, drecv,
):
    branch = lax.axis_index("branch")
    q = lax.axis_index("query")
    core = lax.rem(branch, 2)
    zlo = lax.div(branch, 2)
    zhi, xy = lax.div(q, 16), lax.rem(q, 16)
    x, y = lax.div(xy, 4), lax.rem(xy, 4)
    scale = 1.0 / 32.0
    rows = bw.shape[1] // CHUNKS
    base = core * 64 + zlo * 32
    mine = base + q

    xs = [lax.rem(x + o, 4) * 4 for o in range(4)]
    ys = [lax.rem(y + o, 4) for o in range(4)]
    away = sorted(((i, j) for i in range(4) for j in range(4)), key=lambda t: -(t[0] != 0) - (t[0] == 2) - (t[1] != 0) - (t[1] == 2))
    plane = [xs[i] + ys[j] for i, j in away]
    here, there = zhi * 16, (1 - zhi) * 16
    near = [(branch, here + p) for p in plane[:-1]]
    cross = [(branch, there + p) for p in plane]
    beside = [((1 - zlo) * 2 + core, here + p) for p in plane]
    group = [d for pair in zip(cross, near + [None]) for d in pair if d is not None]
    wide = [d for pair in zip(beside, near + [None]) for d in pair if d is not None]
    partner = (zlo * 2 + (1 - core), q)

    def wcopy(k, c):
        part = pl.ds(c * rows, rows)
        return pltpu.make_async_copy(bw.at[k, part], wbuf.at[k, part], wsem.at[k, c])

    smalls = ((sens_hbm, sens), (bb_hbm, bb), (coords_hbm, coords.at[0]), (fidx_hbm, fidx.at[0]),
              (targ_hbm, targ.at[0]), (w1_hbm, w1), (b1_hbm, b1), (b2_hbm, b2))
    loads = [pltpu.make_async_copy(a, b, insem.at[i]) for i, (a, b) in enumerate(smalls)]
    loads[0].start()
    wcopy(0, 0).start()
    for load in loads[1:]:
        load.start()
    for k in range(3):
        for c in range(CHUNKS):
            if k + c:
                wcopy(k, c).start()
    w2copy = pltpu.make_async_copy(w2, w2buf, w2sem)
    w2copy.start()

    barrier = pltpu.get_barrier_semaphore()
    greeted = group + beside + [partner]
    for device in greeted:
        pl.semaphore_signal(barrier, inc=1, device_id=device, device_id_type=pl.DeviceIdType.MESH)

    def send(source, target, send_sem, recv_sem, device):
        pltpu.make_async_remote_copy(
            src_ref=source, dst_ref=target, send_sem=send_sem, recv_sem=recv_sem,
            device_id=device, device_id_type=pl.DeviceIdType.MESH,
        ).start()

    def wait(ref, sem):
        pltpu.make_async_copy(ref, ref, sem).wait()

    def handed(ref, i, device):
        return pltpu.make_async_remote_copy(
            src_ref=ref[0], dst_ref=ref[1], send_sem=dsend.at[i], recv_sem=drecv.at[i],
            device_id=device, device_id_type=pl.DeviceIdType.MESH,
        )

    def swap(buf, i):
        half = buf.at[pl.ds(core * 64, 64)]
        return handed((half, half), i, partner)

    def aside(buf, i):
        part = buf.at[pl.ds(base, 32)]
        return handed((part, part), i, ((1 - zlo) * 2 + core, q))

    across = [
        handed((r.at[0], r.at[1]), i, (branch, there + xy)) for i, r in enumerate((coords, fidx, targ))
    ]

    loads[0].wait()
    loads[1].wait()
    for k in range(3):
        pre = bb[k : k + 1, :]
        for c in range(CHUNKS):
            wcopy(k, c).wait()
            pre = pre + nn(sens[k : k + 1, c * rows : (c + 1) * rows], wbuf[k, c * rows : (c + 1) * rows, :])
        lat = jnp.tanh(pre).astype(BF16).astype(F32)
        for j in range(8):
            row8[k, j : j + 1, :] = lat[:, 128 * j : 128 * (j + 1)]
        latbuf[mine, k] = row8[k].astype(BF16)
    own = (row8[0] * row8[1] * row8[2]).astype(BF16)
    prodsend[...] = own
    prodbuf[q] = own
    for load in loads[2:]:
        load.wait()

    pl.semaphore_wait(barrier, len(greeted))

    for device in group:
        send(prodsend, prodbuf.at[q], psend, precv, device)
    for copy in across:
        copy.start()
    for device in group:
        send(latbuf.at[mine], latbuf.at[mine], lsend, lrecv, device)

    for k in range(3):
        sk = sens[k : k + 1, :].astype(F32)
        for j in range(16):
            sgf[4 * j + k : 4 * j + k + 1, :] = sk[:, 128 * j : 128 * (j + 1)]
    for j in range(16):
        sensend[j] = sgf[4 * j : 4 * j + 4, :].astype(BF16)
    sgbuf[mine] = sensend[lax.div(q, 2)]

    def layer(which):
        for r in range(4):
            h = jnp.tanh(tn(coords[which, :, 128 * r : 128 * (r + 1)], w1[...]) + b1[...]).astype(BF16)
            at = 512 * which + 128 * r
            hid[at : at + 128, :] = h
            hw = h.astype(F32)
            omh[at : at + 128, :] = (1.0 - hw * hw).astype(BF16)

    layer(0)
    for device in group:
        send(sensend.at[lax.div(device[1], 2)], sgbuf.at[mine], ssend, srecv, device)
    for copy in across:
        copy.wait()
    layer(1)

    def points(ref):
        return jnp.concatenate([ref[0], ref[1]], axis=1)

    owned = lax.broadcasted_iota(jnp.int32, (32, 1024), 0) == points(fidx)
    target = points(targ)
    cf = points(coords).astype(F32)

    w2copy.wait()
    wait(prodbuf.at[pl.ds(0, 31)], precv)
    for f in range(32):
        pf[8 * f : 8 * f + 8, :] = prodbuf[f].astype(F32)
    prod = jnp.concatenate([pf[pl.ds(j, 32, stride=8), :] for j in range(8)], axis=1)
    shift = jnp.sum(prod * b2[...], axis=1, keepdims=True)
    quad = nt(prod.astype(BF16), w2buf[...])
    qh, ql = split(quad)
    dots = nt(jnp.concatenate([qh, ql], axis=0), hid[...])
    dots = dots[:32] + dots[32:] + shift
    pred = jnp.sum(jnp.where(owned, dots, 0.0), axis=0, keepdims=True) * scale
    resid = (pred - target) * (1.0 / 128.0)
    a = jnp.where(owned, resid * scale, 0.0)
    ah, al = split(a)
    hsum = nn(jnp.concatenate([ah, al], axis=0), hid[...])
    hsum = hsum[:32] + hsum[32:]
    asum = jnp.sum(a, axis=1, keepdims=True)
    za = jnp.concatenate([a * cf[c : c + 1, :] for c in range(3)] + [a], axis=0).astype(BF16)
    z = nn(za, omh[...])
    gw1 = [jnp.sum(quad * z[32 * c : 32 * c + 32, :], axis=0, keepdims=True) for c in range(4)]
    for j in range(8):
        msgf[pl.ds(j, 32, stride=16), :] = hsum[:, 128 * j : 128 * (j + 1)]
        for c in range(4):
            at = 16 * (8 * c + j) + 8
            msgf[at : at + 1, :] = gw1[c][:, 128 * j : 128 * (j + 1)]
    sh, sl = split(asum)
    msgf[pl.ds(9, 32, stride=16), :] = jnp.broadcast_to(sh.astype(F32), (32, 128))
    msgf[pl.ds(10, 32, stride=16), :] = jnp.broadcast_to(sl.astype(F32), (32, 128))
    msgf[pl.ds(11, 32, stride=16), :] = jnp.zeros((32, 128), F32)
    for f in range(32):
        msg[f] = msgf[16 * f : 16 * f + ROWS, :].astype(BF16)

    for device in near:
        send(msg.at[pl.ds(lax.rem(device[1], 16) * 2, 2)], rsbuf.at[xy], rsend, rrecv, device)
    rsbuf[xy] = msg[pl.ds(xy * 2, 2)]

    wait(latbuf.at[pl.ds(0, 31)], lrecv)
    wait(sgbuf.at[pl.ds(0, 31)], srecv)
    side_lat, side_sens = aside(latbuf, 3), aside(sgbuf, 4)
    side_lat.start()
    side_sens.start()

    wait(rsbuf.at[pl.ds(0, 15)], rrecv)
    total = rsbuf[0].astype(F32)
    for f in range(1, 16):
        total = total + rsbuf[f].astype(F32)
    first = base + xy * 2
    for r in range(2):
        at = 16 * r
        hf[at : at + ROWS, :] = total[r]
        s = hf[at + 9 : at + 10, :] + hf[at + 10 : at + 11, :]
        sh = s.astype(BF16).astype(F32)
        hf[at + 9 : at + 10, :] = sh
        hf[at + 10 : at + 11, :] = s - sh
        agbuf[first + r] = hf[at : at + ROWS, :].astype(BF16)
    pair = agbuf.at[pl.ds(first, 2)]
    for device in wide:
        send(pair, pair, asend, arecv, device)

    side_lat.wait()
    side_sens.wait()
    swap_lat, swap_sens = swap(latbuf, 5), swap(sgbuf, 6)
    swap_lat.start()
    swap_sens.start()
    swap_lat.wait()
    swap_sens.wait()

    def spread(i, carry):
        at = pl.multiple_of(i * 8, 8)
        for k in range(3):
            lf[k, pl.ds(at, 8), :] = latbuf[i, k].astype(F32)
        return carry

    lax.fori_loop(0, 128, spread, 0, unroll=4)

    def spread_sens(i, carry):
        sgf[pl.ds(i * 4, 4), :] = sgbuf[i].astype(F32)
        return carry

    lax.fori_loop(0, 128, spread_sens, 0, unroll=4)
    odd = lax.rem(q, 2) == 1
    for k in range(3):
        cols = sgf[pl.ds(k, 128, stride=4), :]
        sg_out[k] = jnp.where(odd, pltpu.roll(cols, 64, 1), cols).astype(BF16)
    for j in range(8):
        l0, l1, l2 = [lf[k, pl.ds(j, 128, stride=8), :] for k in range(3)]
        cols = slice(128 * j, 128 * (j + 1))
        m12, m02, m01 = l1 * l2, l0 * l2, l0 * l1
        p_out[:, cols] = (m01 * l2).astype(BF16)
        d_scr[0, :, cols] = m12 * (1.0 - l0 * l0)
        d_scr[1, :, cols] = m02 * (1.0 - l1 * l1)
        d_scr[2, :, cols] = m01 * (1.0 - l2 * l2)

    wait(agbuf.at[pl.ds(0, 62)], arecv)
    swap_h = swap(agbuf, 7)
    swap_h.start()

    def finish(half):
        start = pl.multiple_of(half * 64, 64)

        def spread_h(i, carry):
            at = pl.multiple_of(i * 16, 16)
            hf[pl.ds(at, ROWS), :] = agbuf[start + i].astype(F32)
            return carry

        lax.fori_loop(0, 64, spread_h, 0, unroll=4)
        hm = jnp.concatenate([hf[pl.ds(j, 64, stride=16), :].astype(BF16) for j in range(8)], axis=1)
        sums = hf[pl.ds(9, 64, stride=16), :] + hf[pl.ds(10, 64, stride=16), :]
        g = hf[pl.ds(8, 64, stride=16), :]
        part = pl.ds(start, 64)
        hm_out[part, :] = hm
        s_out[part, :] = sums
        gp = nn(hm, w2buf[...]) + sums[:, 0:1] * b2[...]
        for k in range(3):
            delta_out[k, part, :] = (gp * d_scr[k, part, :]).astype(BF16)
        return g[0:32] + g[32:64]

    g_own = finish(core)
    wait(prodbuf.at[pl.ds(0, 31)], psend)
    wait(latbuf.at[pl.ds(0, 31)], lsend)
    wait(sgbuf.at[pl.ds(0, 31)], ssend)
    wait(rsbuf.at[pl.ds(0, 15)], rsend)
    wait(agbuf.at[pl.ds(0, 62)], asend)
    swap_h.wait()
    g_out[...] = g_own + finish(1 - core)


def output_kernel(
    hm, prod, delta, sg, s, g,
    gbw_out, gbb_out, gw1_out, gb1_out, gw2_out, gb2_out,
    gbw, gbb, gw1, gb1, gw2, gb2, sem,
):
    copies = []

    def drain(source, target):
        copies.append(pltpu.make_async_copy(source, target, sem.at[len(copies)]))
        copies[-1].start()

    for c in range(4):
        part = pl.ds(256 * c, 256)
        gw2[256 * c : 256 * (c + 1), :] = tn(hm[:, 256 * c : 256 * (c + 1)], prod[...])
        drain(gw2.at[part], gw2_out.at[part])
    for k in range(3):
        gbw[k] = tn(sg[k], delta[k])[0:64, :]
        drain(gbw.at[k], gbw_out.at[k])
    for k in range(3):
        gbb[k : k + 1, :] = jnp.sum(delta[k].astype(F32), axis=0, keepdims=True)
    gb2[...] = jnp.sum(s[:, 0:1] * prod[...].astype(F32), axis=0, keepdims=True)
    for j in range(8):
        cols = slice(128 * j, 128 * (j + 1))
        for c in range(3):
            gw1[c : c + 1, cols] = g[8 * c + j : 8 * c + j + 1, :]
        gb1[:, cols] = g[24 + j : 25 + j, :]
    drain(gbb, gbb_out)
    drain(gb2, gb2_out)
    drain(gw1, gw1_out)
    drain(gb1, gb1_out)
    for copy in copies:
        copy.wait()


def shards(sensors, branch_w, branch_b, coords, func_index, targets, trunk_w1, trunk_b1, trunk_w2, trunk_b2):
    vmem = pl.BlockSpec(memory_space=pltpu.VMEM)
    hbm = pl.BlockSpec(memory_space=pltpu.HBM)
    shape = jax.ShapeDtypeStruct
    dma = pltpu.SemaphoreType.DMA
    inputs = (
        sensors.reshape(3, 2048), branch_w, branch_b, coords, func_index.reshape(1, 512),
        targets.reshape(1, 512), trunk_w1, trunk_b1.reshape(1, 1024), trunk_w2, trunk_b2.reshape(1, 1024),
    )
    passed = pl.pallas_call(
        exchange_kernel,
        out_shape=(
            shape((128, 1024), BF16), shape((128, 1024), BF16), shape((3, 128, 1024), BF16),
            shape((3, 128, 128), BF16), shape((128, 128), F32), shape((32, 128), F32),
        ),
        in_specs=[hbm] * 10,
        out_specs=(vmem,) * 6,
        scratch_shapes=[
            VMEM((3, 2048), BF16), VMEM((3, 1024), F32), VMEM((2, 3, 512), BF16), VMEM((2, 1, 512), jnp.int32),
            VMEM((2, 1, 512), F32), VMEM((3, 1024), BF16), VMEM((1, 1024), F32), VMEM((1, 1024), F32),
            VMEM((3, 128, 1024), F32),
            VMEM((3, 2048, 1024), BF16), VMEM((1024, 1024), BF16), VMEM((3, 8, 128), F32),
            VMEM((8, 128), BF16), VMEM((32, 8, 128), BF16), VMEM((256, 128), F32),
            VMEM((128, 3, 8, 128), BF16), VMEM((3, 1024, 128), F32),
            VMEM((16, 4, 128), BF16), VMEM((128, 4, 128), BF16), VMEM((512, 128), F32),
            VMEM((1024, 1024), BF16), VMEM((1024, 1024), BF16),
            VMEM((512, 128), F32), VMEM((32, ROWS, 128), BF16), VMEM((16, 2, ROWS, 128), BF16),
            VMEM((128, ROWS, 128), BF16), VMEM((1024, 128), F32),
            dma((8,)), dma((3, CHUNKS)), dma, dma, dma, dma, dma, dma, dma, dma, dma, dma, dma,
            dma((8,)), dma((8,)),
        ],
        compiler_params=pltpu.CompilerParams(
            collective_id=0, has_side_effects=True, vmem_limit_bytes=40 * 1024 * 1024
        ),
        name="exchange",
    )(*[pltpu.with_memory_space_constraint(v, pltpu.HBM) for v in inputs])
    results = (
        shape((3, 64, 1024), F32), shape((3, 1024), F32), shape((3, 1024), F32),
        shape((1, 1024), F32), shape((1024, 1024), F32), shape((1, 1024), F32),
    )
    gbw, gbb, gw1, gb1, gw2, gb2 = pl.pallas_call(
        output_kernel,
        out_shape=results,
        in_specs=[vmem] * 6,
        out_specs=(hbm,) * 6,
        scratch_shapes=[VMEM(r.shape, F32) for r in results] + [dma((11,))],
        compiler_params=pltpu.CompilerParams(vmem_limit_bytes=16 * 1024 * 1024),
        name="outputs",
    )(*passed)
    return gbw, gbb, gw1, gb1.reshape(1024), gw2, gb2.reshape(1024)


def solution(mesh):
    both = ("branch", "query")
    placed = (P(None, both, None), P(), P(), P(None, both), P(both), P(both), P(), P(), P(), P())
    return jax.shard_map(
        shards,
        mesh=mesh,
        in_specs=placed,
        out_specs=(P(None, "query", None), P(), P(), P(), P(), P()),
        check_vma=False,
    )
```

```python
import jax
import jax.numpy as jnp
from jax import lax
from jax.experimental import pallas as pl
from jax.experimental.pallas import tpu as pltpu
from jax.sharding import PartitionSpec as P

F32 = jnp.float32
BF16 = jnp.bfloat16
ROWS = 10
CHUNKS = 4
VMEM = pltpu.VMEM


def nt(a, b):
    return lax.dot_general(a, b, (((1,), (1,)), ((), ())), preferred_element_type=F32)


def tn(a, b):
    return lax.dot_general(a, b, (((0,), (0,)), ((), ())), preferred_element_type=F32)


def nn(a, b):
    return lax.dot_general(a, b, (((1,), (0,)), ((), ())), preferred_element_type=F32)


def split(x):
    high = x.astype(BF16)
    return high, (x - high.astype(F32)).astype(BF16)


def exchange_kernel(
    sens_hbm, bw, bb_hbm, coords_hbm, fidx_hbm, targ_hbm, w1_hbm, b1_hbm, w2, b2_hbm,
    hm_out, p_out, d_out, sg_out, s_out, g_out, w2buf, b2,
    sens, bb, coords, fidx, targ, w1, b1,
    wbuf, row8, prodsend, prodbuf, pf, latbuf, lf, sensend, sgbuf, sgf,
    hid, omh, msgf, msg, rsbuf, agbuf, hf, tmsg, trs, tag,
    insem, wsem, w2sem, psend, precv, lsend, lrecv, ssend, srecv, rsend, rrecv, asend, arecv,
    tsend, trecv, usend, urecv, dsend, drecv,
):
    branch = lax.axis_index("branch")
    q = lax.axis_index("query")
    core = lax.rem(branch, 2)
    zlo = lax.div(branch, 2)
    zhi, xy = lax.div(q, 16), lax.rem(q, 16)
    x, y = lax.div(xy, 4), lax.rem(xy, 4)
    scale = 1.0 / 32.0
    rows = bw.shape[1] // CHUNKS
    base = core * 64 + zlo * 32
    mine = base + q

    xs = [lax.rem(x + o, 4) * 4 for o in range(4)]
    ys = [lax.rem(y + o, 4) for o in range(4)]
    away = sorted(((i, j) for i in range(4) for j in range(4)), key=lambda t: -(t[0] != 0) - (t[0] == 2) - (t[1] != 0) - (t[1] == 2))
    plane = [xs[i] + ys[j] for i, j in away]
    here, there = zhi * 16, (1 - zhi) * 16
    near = [(branch, here + p) for p in plane[:-1]]
    cross = [(branch, there + p) for p in plane]
    other = (1 - zlo) * 2 + core
    beside = [(other, here + p) for p in plane]
    group = [d for pair in zip(cross, near + [None]) for d in pair if d is not None]
    wide = [d for pair in zip(beside, near + [None]) for d in pair if d is not None]
    partner = (zlo * 2 + (1 - core), q)

    def wcopy(k, c):
        part = pl.ds(c * rows, rows)
        return pltpu.make_async_copy(bw.at[k, part], wbuf.at[k, part], wsem.at[k, c])

    smalls = ((sens_hbm, sens), (bb_hbm, bb), (coords_hbm, coords.at[0]), (fidx_hbm, fidx.at[0]),
              (targ_hbm, targ.at[0]), (w1_hbm, w1), (b1_hbm, b1), (b2_hbm, b2))
    loads = [pltpu.make_async_copy(a, b, insem.at[i]) for i, (a, b) in enumerate(smalls)]
    loads[0].start()
    wcopy(0, 0).start()
    for load in loads[1:]:
        load.start()
    for k in range(3):
        for c in range(CHUNKS):
            if k + c:
                wcopy(k, c).start()
    w2copy = pltpu.make_async_copy(w2, w2buf, w2sem)
    w2copy.start()

    barrier = pltpu.get_barrier_semaphore()
    greeted = group + beside + [(other, there + xy), partner]
    for device in greeted:
        pl.semaphore_signal(barrier, inc=1, device_id=device, device_id_type=pl.DeviceIdType.MESH)

    def send(source, target, send_sem, recv_sem, device):
        pltpu.make_async_remote_copy(
            src_ref=source, dst_ref=target, send_sem=send_sem, recv_sem=recv_sem,
            device_id=device, device_id_type=pl.DeviceIdType.MESH,
        ).start()

    def wait(ref, sem):
        pltpu.make_async_copy(ref, ref, sem).wait()

    def handed(ref, i, device):
        return pltpu.make_async_remote_copy(
            src_ref=ref[0], dst_ref=ref[1], send_sem=dsend.at[i], recv_sem=drecv.at[i],
            device_id=device, device_id_type=pl.DeviceIdType.MESH,
        )

    def swap(buf, i, count=64):
        half = buf.at[pl.ds(core * count, count)]
        return handed((half, half), i, partner)

    def aside(buf, i, start, count, where):
        part = buf.at[pl.ds(start, count)]
        return handed((part, part), i, (other, where + xy))

    across = [
        handed((r.at[0], r.at[1]), i, (branch, there + xy)) for i, r in enumerate((coords, fidx, targ))
    ]

    loads[0].wait()
    loads[1].wait()
    for k in range(3):
        pre = bb[k : k + 1, :]
        for c in range(CHUNKS):
            wcopy(k, c).wait()
            pre = pre + nn(sens[k : k + 1, c * rows : (c + 1) * rows], wbuf[k, c * rows : (c + 1) * rows, :])
        lat = jnp.tanh(pre).astype(BF16).astype(F32)
        for j in range(8):
            row8[k, j : j + 1, :] = lat[:, 128 * j : 128 * (j + 1)]
        latbuf[mine, k] = row8[k].astype(BF16)
    own = (row8[0] * row8[1] * row8[2]).astype(BF16)
    prodsend[...] = own
    prodbuf[q] = own
    for load in loads[2:]:
        load.wait()

    pl.semaphore_wait(barrier, len(greeted))

    for device in group:
        send(prodsend, prodbuf.at[q], psend, precv, device)
    for copy in across:
        copy.start()
    for device in group:
        send(latbuf.at[mine], latbuf.at[mine], lsend, lrecv, device)

    for k in range(3):
        sk = sens[k : k + 1, :].astype(F32)
        for j in range(16):
            sgf[4 * j + k : 4 * j + k + 1, :] = sk[:, 128 * j : 128 * (j + 1)]
    for j in range(16):
        sensend[j] = sgf[4 * j : 4 * j + 4, :].astype(BF16)
    sgbuf[mine] = sensend[lax.div(q, 2)]

    def layer(which):
        for r in range(4):
            h = jnp.tanh(tn(coords[which, :, 128 * r : 128 * (r + 1)], w1[...]) + b1[...]).astype(BF16)
            at = 512 * which + 128 * r
            hid[at : at + 128, :] = h
            hw = h.astype(F32)
            omh[at : at + 128, :] = (1.0 - hw * hw).astype(BF16)

    layer(0)
    for device in group:
        send(sensend.at[lax.div(device[1], 2)], sgbuf.at[mine], ssend, srecv, device)
    for copy in across:
        copy.wait()
    layer(1)

    def points(ref):
        return jnp.concatenate([ref[0], ref[1]], axis=1)

    owned = lax.broadcasted_iota(jnp.int32, (32, 1024), 0) == points(fidx)
    target = points(targ)
    cf = points(coords).astype(F32)

    w2copy.wait()
    wait(prodbuf.at[pl.ds(0, 31)], precv)
    for f in range(32):
        pf[8 * f : 8 * f + 8, :] = prodbuf[f].astype(F32)
    prod = jnp.concatenate([pf[pl.ds(j, 32, stride=8), :] for j in range(8)], axis=1)
    shift = jnp.sum(prod * b2[...], axis=1, keepdims=True)
    quad = nt(prod.astype(BF16), w2buf[...])
    qh, ql = split(quad)
    dots = nt(jnp.concatenate([qh, ql], axis=0), hid[...])
    dots = dots[:32] + dots[32:] + shift

    wait(sgbuf.at[pl.ds(0, 31)], srecv)
    wait(latbuf.at[pl.ds(0, 31)], lrecv)
    sides = [
        aside(sgbuf, 3, base, 32, here),
        aside(latbuf, 4, base + here, 16, here),
        aside(latbuf, 5, base + here, 16, there),
    ]
    for copy in sides:
        copy.start()

    pred = jnp.sum(jnp.where(owned, dots, 0.0), axis=0, keepdims=True) * scale
    resid = (pred - target) * (1.0 / 128.0)
    a = jnp.where(owned, resid * scale, 0.0)
    ah, al = split(a)
    hsum = nn(jnp.concatenate([ah, al], axis=0), hid[...])
    hsum = hsum[:32] + hsum[32:]
    asum = jnp.sum(a, axis=1, keepdims=True)
    for j in range(8):
        msgf[pl.ds(j, 32, stride=16), :] = hsum[:, 128 * j : 128 * (j + 1)]
    sh, sl = split(asum)
    msgf[pl.ds(8, 32, stride=16), :] = jnp.broadcast_to(sh.astype(F32), (32, 128))
    msgf[pl.ds(9, 32, stride=16), :] = jnp.broadcast_to(sl.astype(F32), (32, 128))
    for f in range(32):
        msg[f] = msgf[16 * f : 16 * f + ROWS, :].astype(BF16)

    for device in near:
        send(msg.at[pl.ds(lax.rem(device[1], 16) * 2, 2)], rsbuf.at[xy], rsend, rrecv, device)
    rsbuf[xy] = msg[pl.ds(xy * 2, 2)]

    za = jnp.concatenate([a * cf[c : c + 1, :] for c in range(3)] + [a], axis=0).astype(BF16)
    z = nn(za, omh[...])
    for c in range(4):
        row = jnp.sum(quad * z[32 * c : 32 * c + 32, :], axis=0, keepdims=True)
        for j in range(8):
            tmsg[4 * c + j // 2, j % 2 : j % 2 + 1, :] = row[:, 128 * j : 128 * (j + 1)]
    for device in near:
        send(tmsg.at[lax.rem(device[1], 16)], trs.at[xy], tsend, trecv, device)
    trs[xy] = tmsg[xy]

    wait(rsbuf.at[pl.ds(0, 15)], rrecv)
    total = rsbuf[0].astype(F32)
    for f in range(1, 16):
        total = total + rsbuf[f].astype(F32)
    first = base + xy * 2
    for r in range(2):
        at = 16 * r
        hf[at : at + ROWS, :] = total[r]
        s = hf[at + 8 : at + 9, :] + hf[at + 9 : at + 10, :]
        sh = s.astype(BF16).astype(F32)
        hf[at + 8 : at + 9, :] = sh
        hf[at + 9 : at + 10, :] = s - sh
        agbuf[first + r] = hf[at : at + ROWS, :].astype(BF16)
    pair = agbuf.at[pl.ds(first, 2)]
    for device in wide:
        send(pair, pair, asend, arecv, device)

    for copy in sides:
        copy.wait()
    swap_lat, swap_sens = swap(latbuf, 6), swap(sgbuf, 7)
    swap_lat.start()
    swap_sens.start()

    wait(trs.at[pl.ds(0, 15)], trecv)
    tsum = trs[0]
    for f in range(1, 16):
        tsum = tsum + trs[f]
    tmine = tag.at[core * 32 + zlo * 16 + xy]
    tmine[...] = tsum
    for device in wide:
        send(tmine, tmine, usend, urecv, device)

    swap_lat.wait()
    swap_sens.wait()

    def spread(i, carry):
        at = pl.multiple_of(i * 8, 8)
        for k in range(3):
            lf[k, pl.ds(at, 8), :] = latbuf[i, k].astype(F32)
        return carry

    lax.fori_loop(0, 128, spread, 0, unroll=4)

    def spread_sens(i, carry):
        sgf[pl.ds(i * 4, 4), :] = sgbuf[i].astype(F32)
        return carry

    lax.fori_loop(0, 128, spread_sens, 0, unroll=4)
    odd = lax.rem(q, 2) == 1
    for k in range(3):
        cols = sgf[pl.ds(k, 128, stride=4), :]
        sg_out[k] = jnp.where(odd, pltpu.roll(cols, 64, 1), cols).astype(BF16)
    for j in range(8):
        l0, l1, l2 = [lf[k, pl.ds(j, 128, stride=8), :] for k in range(3)]
        cols = slice(128 * j, 128 * (j + 1))
        m12, m02, m01 = l1 * l2, l0 * l2, l0 * l1
        p_out[:, cols] = (m01 * l2).astype(BF16)
        d_out[0, :, cols] = m12 * (1.0 - l0 * l0)
        d_out[1, :, cols] = m02 * (1.0 - l1 * l1)
        d_out[2, :, cols] = m01 * (1.0 - l2 * l2)

    wait(agbuf.at[pl.ds(0, 62)], arecv)
    swap_h = swap(agbuf, 8)
    swap_h.start()

    def arrange(half):
        start = pl.multiple_of(half * 64, 64)

        def spread_h(i, carry):
            at = pl.multiple_of(i * 16, 16)
            hf[pl.ds(at, ROWS), :] = agbuf[start + i].astype(F32)
            return carry

        lax.fori_loop(0, 64, spread_h, 0, unroll=8)
        part = pl.ds(start, 64)
        for j in range(8):
            hm_out[part, 128 * j : 128 * (j + 1)] = hf[pl.ds(j, 64, stride=16), :].astype(BF16)
        s_out[part, :] = hf[pl.ds(8, 64, stride=16), :] + hf[pl.ds(9, 64, stride=16), :]

    arrange(core)
    wait(tag.at[pl.ds(0, 31)], urecv)
    swap_t = swap(tag, 9, 32)
    swap_t.start()
    wait(prodbuf.at[pl.ds(0, 31)], psend)
    wait(latbuf.at[pl.ds(0, 31)], lsend)
    wait(sgbuf.at[pl.ds(0, 31)], ssend)
    wait(rsbuf.at[pl.ds(0, 15)], rsend)
    wait(trs.at[pl.ds(0, 15)], tsend)
    wait(agbuf.at[pl.ds(0, 62)], asend)
    wait(tag.at[pl.ds(0, 31)], usend)
    swap_h.wait()
    arrange(1 - core)
    swap_t.wait()
    g_out[...] = (tag[0:16] + tag[16:32]) + (tag[32:48] + tag[48:64])


def output_kernel(
    hm, prod, d, sg, s, g, w2, b2,
    gbw_out, gbb_out, gw1_out, gb1_out, gw2_out, gb2_out,
    gbw, gbb, gw1, gb1, gw2, gb2, sem,
):
    copies = []

    def drain(source, target):
        copies.append(pltpu.make_async_copy(source, target, sem.at[len(copies)]))
        copies[-1].start()

    def trunk(c):
        part = pl.ds(256 * c, 256)
        gw2[256 * c : 256 * (c + 1), :] = tn(hm[:, 256 * c : 256 * (c + 1)], prod[...])
        drain(gw2.at[part], gw2_out.at[part])

    trunk(0)
    trunk(1)
    sums = s[:, 0:1]
    gp = nn(hm[...], w2[...]) + sums * b2[...]
    trunk(2)
    trunk(3)
    for k in range(3):
        delta = (gp * d[k]).astype(BF16)
        gbw[k] = tn(sg[k], delta)[0:64, :]
        drain(gbw.at[k], gbw_out.at[k])
        gbb[k : k + 1, :] = jnp.sum(delta.astype(F32), axis=0, keepdims=True)
    drain(gbb, gbb_out)
    gb2[...] = jnp.sum(sums * prod[...].astype(F32), axis=0, keepdims=True)
    drain(gb2, gb2_out)
    for j in range(8):
        cols = slice(128 * j, 128 * (j + 1))
        for c in range(3):
            gw1[c : c + 1, cols] = g[4 * c + j // 2, j % 2 : j % 2 + 1, :]
        gb1[:, cols] = g[12 + j // 2, j % 2 : j % 2 + 1, :]
    drain(gw1, gw1_out)
    drain(gb1, gb1_out)
    for copy in copies:
        copy.wait()


def shards(sensors, branch_w, branch_b, coords, func_index, targets, trunk_w1, trunk_b1, trunk_w2, trunk_b2):
    vmem = pl.BlockSpec(memory_space=pltpu.VMEM)
    hbm = pl.BlockSpec(memory_space=pltpu.HBM)
    shape = jax.ShapeDtypeStruct
    dma = pltpu.SemaphoreType.DMA
    inputs = (
        sensors.reshape(3, 2048), branch_w, branch_b, coords, func_index.reshape(1, 512),
        targets.reshape(1, 512), trunk_w1, trunk_b1.reshape(1, 1024), trunk_w2, trunk_b2.reshape(1, 1024),
    )
    passed = pl.pallas_call(
        exchange_kernel,
        out_shape=(
            shape((128, 1024), BF16), shape((128, 1024), BF16), shape((3, 128, 1024), F32),
            shape((3, 128, 128), BF16), shape((128, 128), F32), shape((16, 2, 128), F32),
            shape((1024, 1024), BF16), shape((1, 1024), F32),
        ),
        in_specs=[hbm] * 10,
        out_specs=(vmem,) * 8,
        scratch_shapes=[
            VMEM((3, 2048), BF16), VMEM((3, 1024), F32), VMEM((2, 3, 512), BF16), VMEM((2, 1, 512), jnp.int32),
            VMEM((2, 1, 512), F32), VMEM((3, 1024), BF16), VMEM((1, 1024), F32),
            VMEM((3, 2048, 1024), BF16), VMEM((3, 8, 128), F32),
            VMEM((8, 128), BF16), VMEM((32, 8, 128), BF16), VMEM((256, 128), F32),
            VMEM((128, 3, 8, 128), BF16), VMEM((3, 1024, 128), F32),
            VMEM((16, 4, 128), BF16), VMEM((128, 4, 128), BF16), VMEM((512, 128), F32),
            VMEM((1024, 1024), BF16), VMEM((1024, 1024), BF16),
            VMEM((512, 128), F32), VMEM((32, ROWS, 128), BF16), VMEM((16, 2, ROWS, 128), BF16),
            VMEM((128, ROWS, 128), BF16), VMEM((1024, 128), F32),
            VMEM((16, 2, 128), F32), VMEM((16, 2, 128), F32), VMEM((64, 2, 128), F32),
            dma((8,)), dma((3, CHUNKS)), dma, dma, dma, dma, dma, dma, dma, dma, dma, dma, dma,
            dma, dma, dma, dma, dma((10,)), dma((10,)),
        ],
        compiler_params=pltpu.CompilerParams(
            collective_id=0, has_side_effects=True, vmem_limit_bytes=40 * 1024 * 1024
        ),
        name="exchange",
    )(*[pltpu.with_memory_space_constraint(v, pltpu.HBM) for v in inputs])
    results = (
        shape((3, 64, 1024), F32), shape((3, 1024), F32), shape((3, 1024), F32),
        shape((1, 1024), F32), shape((1024, 1024), F32), shape((1, 1024), F32),
    )
    gbw, gbb, gw1, gb1, gw2, gb2 = pl.pallas_call(
        output_kernel,
        out_shape=results,
        in_specs=[vmem] * 8,
        out_specs=(hbm,) * 6,
        scratch_shapes=[VMEM(r.shape, F32) for r in results] + [dma((11,))],
        compiler_params=pltpu.CompilerParams(vmem_limit_bytes=16 * 1024 * 1024),
        name="outputs",
    )(*passed)
    return gbw, gbb, gw1, gb1.reshape(1024), gw2, gb2.reshape(1024)


def solution(mesh):
    both = ("branch", "query")
    placed = (P(None, both, None), P(), P(), P(None, both), P(both), P(both), P(), P(), P(), P())
    return jax.shard_map(
        shards,
        mesh=mesh,
        in_specs=placed,
        out_specs=(P(None, "query", None), P(), P(), P(), P(), P()),
        check_vma=False,
    )
```

```python
import jax
import jax.numpy as jnp
from jax import lax
from jax.experimental import pallas as pl
from jax.experimental.pallas import tpu as pltpu
from jax.sharding import PartitionSpec as P

F32 = jnp.float32
BF16 = jnp.bfloat16
CHUNKS = 2
VMEM = pltpu.VMEM


def nt(a, b):
    return lax.dot_general(a, b, (((1,), (1,)), ((), ())), preferred_element_type=F32)


def tn(a, b):
    return lax.dot_general(a, b, (((0,), (0,)), ((), ())), preferred_element_type=F32)


def nn(a, b):
    return lax.dot_general(a, b, (((1,), (0,)), ((), ())), preferred_element_type=F32)


def split(x):
    high = x.astype(BF16)
    return high, (x - high.astype(F32)).astype(BF16)


def exchange_kernel(
    sens_hbm, bw, bb_hbm, coords_hbm, fidx_hbm, targ_hbm, w1_hbm, b1_hbm, w2, b2_hbm,
    hm_out, p_out, d_out, sg_out, s_out, g_out, w2buf, b2,
    sens, bb, coords, fidx, targ, w1, b1,
    wbuf, row8, prodsend, prodbuf, pf, latbuf, lf, sensend, sgbuf, sgf,
    hid, omh, msgf, msg, rsbuf, agbuf, hf, tmsg, trs, tag, tf, srow,
    insem, wsem, w2sem, psend, precv, lsend, lrecv, ssend, srecv, rsend, rrecv, asend, arecv,
    tsend, trecv, usend, urecv, dsend, drecv,
):
    branch = lax.axis_index("branch")
    q = lax.axis_index("query")
    core = lax.rem(branch, 2)
    zlo = lax.div(branch, 2)
    zhi, xy = lax.div(q, 16), lax.rem(q, 16)
    x, y = lax.div(xy, 4), lax.rem(xy, 4)
    scale = 1.0 / 32.0
    rows = bw.shape[1] // CHUNKS
    base = core * 64 + zlo * 32
    mine = base + q

    xs = [lax.rem(x + o, 4) * 4 for o in range(4)]
    ys = [lax.rem(y + o, 4) for o in range(4)]
    away = sorted(((i, j) for i in range(4) for j in range(4)), key=lambda t: -(t[0] != 0) - (t[0] == 2) - (t[1] != 0) - (t[1] == 2))
    plane = [xs[i] + ys[j] for i, j in away]
    here, there = zhi * 16, (1 - zhi) * 16
    near = [(branch, here + p) for p in plane[:-1]]
    cross = [(branch, there + p) for p in plane]
    other = (1 - zlo) * 2 + core
    beside = [(other, here + p) for p in plane]
    group = [d for pair in zip(cross, near + [None]) for d in pair if d is not None]
    wide = [d for pair in zip(beside, near + [None]) for d in pair if d is not None]
    partner = (zlo * 2 + (1 - core), q)

    def wcopy(k, c):
        part = pl.ds(c * rows, rows)
        return pltpu.make_async_copy(bw.at[k, part], wbuf.at[k, part], wsem.at[k, c])

    smalls = ((sens_hbm, sens), (bb_hbm, bb), (coords_hbm, coords.at[0]), (fidx_hbm, fidx.at[0]),
              (targ_hbm, targ.at[0]), (w1_hbm, w1), (b1_hbm, b1), (b2_hbm, b2))
    loads = [pltpu.make_async_copy(a, b, insem.at[i]) for i, (a, b) in enumerate(smalls)]
    loads[0].start()
    wcopy(0, 0).start()
    for load in loads[1:]:
        load.start()
    for k in range(3):
        for c in range(CHUNKS):
            if k + c:
                wcopy(k, c).start()
    w2copy = pltpu.make_async_copy(w2, w2buf, w2sem)
    w2copy.start()

    barrier = pltpu.get_barrier_semaphore()
    facing = [(b + 1 - 2 * core, p) for b, p in wide] + [partner]
    greeted = group + beside + [(other, there + xy)] + facing
    for device in greeted:
        pl.semaphore_signal(barrier, inc=1, device_id=device, device_id_type=pl.DeviceIdType.MESH)

    def send(source, target, send_sem, recv_sem, device):
        pltpu.make_async_remote_copy(
            src_ref=source, dst_ref=target, send_sem=send_sem, recv_sem=recv_sem,
            device_id=device, device_id_type=pl.DeviceIdType.MESH,
        ).start()

    def wait(ref, sem):
        pltpu.make_async_copy(ref, ref, sem).wait()

    def handed(ref, i, device):
        return pltpu.make_async_remote_copy(
            src_ref=ref[0], dst_ref=ref[1], send_sem=dsend.at[i], recv_sem=drecv.at[i],
            device_id=device, device_id_type=pl.DeviceIdType.MESH,
        )

    def swap(buf, i, count=64):
        half = buf.at[pl.ds(core * count, count)]
        return handed((half, half), i, partner)

    def aside(buf, i, start, count, where):
        part = buf.at[pl.ds(start, count)]
        return handed((part, part), i, (other, where + xy))

    across = [
        handed((r.at[0], r.at[1]), i, (branch, there + xy)) for i, r in enumerate((coords, fidx, targ))
    ]

    loads[0].wait()
    loads[1].wait()
    for k in range(3):
        pre = bb[k : k + 1, :]
        for c in range(CHUNKS):
            wcopy(k, c).wait()
            pre = pre + nn(sens[k : k + 1, c * rows : (c + 1) * rows], wbuf[k, c * rows : (c + 1) * rows, :])
        lat = jnp.tanh(pre).astype(BF16).astype(F32)
        for j in range(8):
            row8[k, j : j + 1, :] = lat[:, 128 * j : 128 * (j + 1)]
        latbuf[mine, k] = row8[k].astype(BF16)
    own = (row8[0] * row8[1] * row8[2]).astype(BF16)
    prodsend[...] = own
    prodbuf[q] = own
    for load in loads[2:]:
        load.wait()

    pl.semaphore_wait(barrier, len(greeted))

    for device in group:
        send(prodsend, prodbuf.at[q], psend, precv, device)
    for copy in across:
        copy.start()
    for device in group:
        send(latbuf.at[mine], latbuf.at[mine], lsend, lrecv, device)

    for k in range(3):
        sk = sens[k : k + 1, :].astype(F32)
        for j in range(16):
            sgf[4 * j + k : 4 * j + k + 1, :] = sk[:, 128 * j : 128 * (j + 1)]
    for j in range(16):
        sensend[j] = sgf[4 * j : 4 * j + 4, :].astype(BF16)
    sgbuf[mine] = sensend[lax.div(q, 2)]

    def layer(which):
        for r in range(4):
            h = jnp.tanh(tn(coords[which, :, 128 * r : 128 * (r + 1)], w1[...]) + b1[...]).astype(BF16)
            at = 512 * which + 128 * r
            hid[at : at + 128, :] = h
            hw = h.astype(F32)
            omh[at : at + 128, :] = (1.0 - hw * hw).astype(BF16)

    layer(0)
    for device in group:
        send(sensend.at[lax.div(device[1], 2)], sgbuf.at[mine], ssend, srecv, device)
    for copy in across:
        copy.wait()
    layer(1)

    def points(ref):
        return jnp.concatenate([ref[0], ref[1]], axis=1)

    owned = lax.broadcasted_iota(jnp.int32, (32, 1024), 0) == points(fidx)
    target = points(targ)
    cf = points(coords).astype(F32)

    w2copy.wait()
    wait(prodbuf.at[pl.ds(0, 31)], precv)
    for f in range(32):
        pf[8 * f : 8 * f + 8, :] = prodbuf[f].astype(F32)
    prod = jnp.concatenate([pf[pl.ds(j, 32, stride=8), :] for j in range(8)], axis=1)
    shift = jnp.sum(prod * b2[...], axis=1, keepdims=True)
    quad = nt(prod.astype(BF16), w2buf[...])
    qh, ql = split(quad)
    dots = nt(jnp.concatenate([qh, ql], axis=0), hid[...])
    dots = dots[:32] + dots[32:] + shift
    pred = jnp.sum(jnp.where(owned, dots, 0.0), axis=0, keepdims=True) * scale
    resid = (pred - target) * (1.0 / 128.0)
    a = jnp.where(owned, resid * scale, 0.0)
    ah, al = split(a)
    hsum = nn(jnp.concatenate([ah, al], axis=0), hid[...])
    hsum = hsum[:32] + hsum[32:]
    for j in range(8):
        msgf[pl.ds(j, 32, stride=8), :] = hsum[:, 128 * j : 128 * (j + 1)]
    for f in range(32):
        msg[f] = msgf[8 * f : 8 * f + 8, :].astype(BF16)

    for device in near:
        send(msg.at[pl.ds(lax.rem(device[1], 16) * 2, 2)], rsbuf.at[xy], rsend, rrecv, device)
    rsbuf[xy] = msg[pl.ds(xy * 2, 2)]

    za = jnp.concatenate([a * cf[c : c + 1, :] for c in range(3)] + [a], axis=0).astype(BF16)
    z = nn(za, omh[...])
    for c in range(4):
        row = jnp.sum(quad * z[32 * c : 32 * c + 32, :], axis=0, keepdims=True)
        for j in range(8):
            at = 4 * (4 * c + j // 2) + j % 2
            tf[at : at + 1, :] = row[:, 128 * j : 128 * (j + 1)]
    srow[...] = jnp.broadcast_to(jnp.sum(a, axis=1, keepdims=True), (32, 128))
    left = lax.broadcasted_iota(jnp.int32, (1, 128), 1) < 64
    for j in range(16):
        s = jnp.where(left, srow[2 * j : 2 * j + 1, :], srow[2 * j + 1 : 2 * j + 2, :])
        sh = s.astype(BF16).astype(F32)
        tf[4 * j + 2 : 4 * j + 3, :] = sh
        tf[4 * j + 3 : 4 * j + 4, :] = s - sh
        tmsg[j] = tf[4 * j : 4 * j + 4, :].astype(BF16)
    for device in near:
        send(tmsg.at[lax.rem(device[1], 16)], trs.at[xy], tsend, trecv, device)
    trs[xy] = tmsg[xy]

    wait(sgbuf.at[pl.ds(0, 31)], srecv)
    wait(latbuf.at[pl.ds(0, 31)], lrecv)
    sides = [
        aside(sgbuf, 3, base, 32, here),
        aside(latbuf, 4, base + here, 16, here),
        aside(latbuf, 5, base + here, 16, there),
    ]
    for copy in sides:
        copy.start()

    wait(rsbuf.at[pl.ds(0, 15)], rrecv)
    total = rsbuf[0].astype(F32)
    for f in range(1, 16):
        total = total + rsbuf[f].astype(F32)
    first = base + xy * 2
    agbuf[pl.ds(first, 2)] = total.astype(BF16)
    pair = agbuf.at[pl.ds(first, 2)]
    for device in wide:
        send(pair, pair, asend, arecv, device)

    wait(trs.at[pl.ds(0, 15)], trecv)
    tsum = trs[0].astype(F32)
    for f in range(1, 16):
        tsum = tsum + trs[f].astype(F32)
    tf[0:4, :] = tsum
    s = tf[2:3, :] + tf[3:4, :]
    sh = s.astype(BF16).astype(F32)
    tf[2:3, :] = sh
    tf[3:4, :] = s - sh
    tmine = tag.at[core * 32 + zlo * 16 + xy]
    tmine[...] = tf[0:4, :].astype(BF16)
    for device in wide + facing:
        send(tmine, tmine, usend, urecv, device)

    for copy in sides:
        copy.wait()
    swap_lat, swap_sens = swap(latbuf, 6), swap(sgbuf, 7)
    swap_lat.start()
    swap_sens.start()
    swap_lat.wait()
    swap_sens.wait()

    def spread(i, carry):
        at = pl.multiple_of(i * 8, 8)
        for k in range(3):
            lf[k, pl.ds(at, 8), :] = latbuf[i, k].astype(F32)
        return carry

    lax.fori_loop(0, 128, spread, 0, unroll=4)

    def spread_sens(i, carry):
        sgf[pl.ds(i * 4, 4), :] = sgbuf[i].astype(F32)
        return carry

    lax.fori_loop(0, 128, spread_sens, 0, unroll=4)
    odd = lax.rem(q, 2) == 1
    for k in range(3):
        cols = sgf[pl.ds(k, 128, stride=4), :]
        sg_out[k] = jnp.where(odd, pltpu.roll(cols, 64, 1), cols).astype(BF16)
    for j in range(8):
        l0, l1, l2 = [lf[k, pl.ds(j, 128, stride=8), :] for k in range(3)]
        cols = slice(128 * j, 128 * (j + 1))
        m12, m02, m01 = l1 * l2, l0 * l2, l0 * l1
        p_out[:, cols] = (m01 * l2).astype(BF16)
        d_out[0, :, cols] = m12 * (1.0 - l0 * l0)
        d_out[1, :, cols] = m02 * (1.0 - l1 * l1)
        d_out[2, :, cols] = m01 * (1.0 - l2 * l2)

    wait(agbuf.at[pl.ds(0, 62)], arecv)
    swap_h = swap(agbuf, 8)
    swap_h.start()

    def arrange(half):
        start = pl.multiple_of(half * 64, 64)

        def spread_h(i, carry):
            at = pl.multiple_of(i * 8, 8)
            hf[pl.ds(at, 8), :] = agbuf[start + i].astype(F32)
            return carry

        lax.fori_loop(0, 64, spread_h, 0, unroll=8)
        for j in range(8):
            hm_out[pl.ds(start, 64), 128 * j : 128 * (j + 1)] = hf[pl.ds(j, 64, stride=8), :].astype(BF16)

    arrange(core)
    wait(prodbuf.at[pl.ds(0, 31)], psend)
    wait(latbuf.at[pl.ds(0, 31)], lsend)
    wait(sgbuf.at[pl.ds(0, 31)], ssend)
    wait(rsbuf.at[pl.ds(0, 15)], rsend)
    wait(trs.at[pl.ds(0, 15)], tsend)
    wait(agbuf.at[pl.ds(0, 62)], asend)
    wait(tag.at[pl.ds(0, 63)], usend)
    wait(tag.at[pl.ds(0, 63)], urecv)
    for i in range(64):
        tf[4 * i : 4 * i + 4, :] = tag[i].astype(F32)
    for r in range(2):
        g = tf[pl.ds(r, 64, stride=4), :]
        g_out[r] = (g[0:16] + g[16:32]) + (g[32:48] + g[48:64])
    s = tf[pl.ds(2, 64, stride=4), :] + tf[pl.ds(3, 64, stride=4), :]
    s_out[pl.ds(0, 64, stride=2), :] = s
    s_out[pl.ds(1, 64, stride=2), :] = pltpu.roll(s, 64, 1)
    swap_h.wait()
    arrange(1 - core)


def output_kernel(
    hm, prod, d, sg, s, g, w2, b2,
    gbw_out, gbb_out, gw1_out, gb1_out, gw2_out, gb2_out,
    gbw, gbb, gw1, gb1, gw2, gb2, sem,
):
    copies = []

    def drain(source, target):
        copies.append(pltpu.make_async_copy(source, target, sem.at[len(copies)]))
        copies[-1].start()

    def trunk(c):
        part = pl.ds(256 * c, 256)
        gw2[256 * c : 256 * (c + 1), :] = tn(hm[:, 256 * c : 256 * (c + 1)], prod[...])
        drain(gw2.at[part], gw2_out.at[part])

    trunk(0)
    trunk(1)
    sums = s[:, 0:1]
    gp = nn(hm[...], w2[...]) + sums * b2[...]
    trunk(2)
    trunk(3)
    for k in range(3):
        delta = (gp * d[k]).astype(BF16)
        gbw[k] = tn(sg[k], delta)[0:64, :]
        drain(gbw.at[k], gbw_out.at[k])
        gbb[k : k + 1, :] = jnp.sum(delta.astype(F32), axis=0, keepdims=True)
    drain(gbb, gbb_out)
    gb2[...] = jnp.sum(sums * prod[...].astype(F32), axis=0, keepdims=True)
    drain(gb2, gb2_out)
    for j in range(8):
        cols = slice(128 * j, 128 * (j + 1))
        for c in range(3):
            gw1[c : c + 1, cols] = g[j % 2, 4 * c + j // 2 : 4 * c + j // 2 + 1, :]
        gb1[:, cols] = g[j % 2, 12 + j // 2 : 13 + j // 2, :]
    drain(gw1, gw1_out)
    drain(gb1, gb1_out)
    for copy in copies:
        copy.wait()


def shards(sensors, branch_w, branch_b, coords, func_index, targets, trunk_w1, trunk_b1, trunk_w2, trunk_b2):
    vmem = pl.BlockSpec(memory_space=pltpu.VMEM)
    hbm = pl.BlockSpec(memory_space=pltpu.HBM)
    shape = jax.ShapeDtypeStruct
    dma = pltpu.SemaphoreType.DMA
    inputs = (
        sensors.reshape(3, 2048), branch_w, branch_b, coords, func_index.reshape(1, 512),
        targets.reshape(1, 512), trunk_w1, trunk_b1.reshape(1, 1024), trunk_w2, trunk_b2.reshape(1, 1024),
    )
    passed = pl.pallas_call(
        exchange_kernel,
        out_shape=(
            shape((128, 1024), BF16), shape((128, 1024), BF16), shape((3, 128, 1024), F32),
            shape((3, 128, 128), BF16), shape((128, 128), F32), shape((2, 16, 128), F32),
            shape((1024, 1024), BF16), shape((1, 1024), F32),
        ),
        in_specs=[hbm] * 10,
        out_specs=(vmem,) * 8,
        scratch_shapes=[
            VMEM((3, 2048), BF16), VMEM((3, 1024), F32), VMEM((2, 3, 512), BF16), VMEM((2, 1, 512), jnp.int32),
            VMEM((2, 1, 512), F32), VMEM((3, 1024), BF16), VMEM((1, 1024), F32),
            VMEM((3, 2048, 1024), BF16), VMEM((3, 8, 128), F32),
            VMEM((8, 128), BF16), VMEM((32, 8, 128), BF16), VMEM((256, 128), F32),
            VMEM((128, 3, 8, 128), BF16), VMEM((3, 1024, 128), F32),
            VMEM((16, 4, 128), BF16), VMEM((128, 4, 128), BF16), VMEM((512, 128), F32),
            VMEM((1024, 1024), BF16), VMEM((1024, 1024), BF16),
            VMEM((256, 128), F32), VMEM((32, 8, 128), BF16), VMEM((16, 2, 8, 128), BF16),
            VMEM((128, 8, 128), BF16), VMEM((512, 128), F32),
            VMEM((16, 4, 128), BF16), VMEM((16, 4, 128), BF16), VMEM((64, 4, 128), BF16),
            VMEM((256, 128), F32), VMEM((32, 128), F32),
            dma((8,)), dma((3, CHUNKS)), dma, dma, dma, dma, dma, dma, dma, dma, dma, dma, dma,
            dma, dma, dma, dma, dma((10,)), dma((10,)),
        ],
        compiler_params=pltpu.CompilerParams(
            collective_id=0, has_side_effects=True, vmem_limit_bytes=40 * 1024 * 1024
        ),
        name="exchange",
    )(*[pltpu.with_memory_space_constraint(v, pltpu.HBM) for v in inputs])
    results = (
        shape((3, 64, 1024), F32), shape((3, 1024), F32), shape((3, 1024), F32),
        shape((1, 1024), F32), shape((1024, 1024), F32), shape((1, 1024), F32),
    )
    gbw, gbb, gw1, gb1, gw2, gb2 = pl.pallas_call(
        output_kernel,
        out_shape=results,
        in_specs=[vmem] * 8,
        out_specs=(hbm,) * 6,
        scratch_shapes=[VMEM(r.shape, F32) for r in results] + [dma((11,))],
        compiler_params=pltpu.CompilerParams(vmem_limit_bytes=16 * 1024 * 1024),
        name="outputs",
    )(*passed)
    return gbw, gbb, gw1, gb1.reshape(1024), gw2, gb2.reshape(1024)


def solution(mesh):
    both = ("branch", "query")
    placed = (P(None, both, None), P(), P(), P(None, both), P(both), P(both), P(), P(), P(), P())
    return jax.shard_map(
        shards,
        mesh=mesh,
        in_specs=placed,
        out_specs=(P(None, "query", None), P(), P(), P(), P(), P()),
        check_vma=False,
    )
```
